256 devices in a mesh: grp: 8 (over z), dev: 32 (over y, x, core).
Axes of the slice: x: 4, y: 4, z: 8, core: 2. Of those that a mesh axis runs over, the one named last changes fastest.
Arguments:
- layer_inputs: bfloat16 [8, 8192, 4096], P(None, 'grp', 'dev')
- output_grads: bfloat16 [8, 8192, 2048], P(None, ('grp', 'dev'))
- layer_owner: int32 [8], replicated, may hold values from 0 to 7, each once
- master_weights: float32 [8, 4096, 2048], P('grp', 'dev')
- momentum: float32 [8, 4096, 2048], P('grp', 'dev'), may hold values from -6 to 6
- table_blocks: float32 [8, 256, 128, 128], P('grp', 'dev'), may hold values from -6 to 6
- block_grads: bfloat16 [8, 32, 64, 128, 128], P('grp', 'dev'), may hold values from -6 to 6
- block_ids: int32 [8, 32, 64], P('grp', 'dev'), may hold values from 0 to 7
- block_counts: int32 [8, 32, 32], P('grp', 'dev'), may hold values from 0 to 2, as said below
Outputs:
- new_master: float32 [8, 4096, 2048], P('grp', 'dev')
- new_momentum: float32 [8, 4096, 2048], P('grp', 'dev')
- new_weights: bfloat16 [8, 4096, 2048], P(None, 'dev')
- new_table: float32 [8, 256, 128, 128], P('grp', 'dev')
The draws below stay inside these ranges and needn't reach their ends.
Inputs may be any that keep to these rules, and one draw needn't show every extreme that they name: `layer_owner`: each group owns exactly one layer. `block_ids`: several live slots may name the same block; their gradients add. `block_counts`: in every group some owners receive 2 live slots from every device; slots at or past the count hold stale data.
All inputs are finite; a program needn't handle non-finite values.
Results may differ from the reference program's by a relative error of at most 0.001.
Values may be sent and summed in bfloat16 or wider, within the bound.
A program may use at most 128 MiB of HBM per device.

```python
import jax
import jax.numpy as jnp
from jax import lax

D = 4096
OUTW = 2048
E = 128
BLK = 128
NB = 8
CAP = 2
LAYERS = 8
TOKENS = 8192
N_GRP = 8
N_DEV = 32


def feature_scale(key, count):
    spread = jax.random.uniform(key, (count,), jnp.float32)
    ramp = jnp.arange(count, dtype=jnp.float32) / count
    return 10.0 ** (spread - 0.5) * 3.0 ** (ramp - 0.5)


def column_scale(key, count):
    spread = jax.random.uniform(key, (count,), jnp.float32)
    return 10.0 ** (0.5 * (spread - 0.5))


def base_values(key, shape):
    first = jax.random.fold_in(key, 0)
    values = jax.random.normal(first, shape, jnp.float32)
    return values


def draw_layer_inputs(key, part):
    first, second = jax.random.split(jax.random.fold_in(key, 11))
    scale = feature_scale(first, D)
    values = base_values(second, (LAYERS, TOKENS, D))
    return (values * scale[None, None, :]).astype(jnp.bfloat16)


def draw_output_grads(key, part):
    first, second = jax.random.split(jax.random.fold_in(key, 23))
    scale = 0.02 * column_scale(first, OUTW)
    values = base_values(second, (LAYERS, TOKENS, OUTW))
    return (values * scale[None, None, :]).astype(jnp.bfloat16)


def draw_master_weights(key, part):
    first, second, third = jax.random.split(jax.random.fold_in(key, 37), 3)
    rows = feature_scale(first, D)
    cols = column_scale(second, OUTW)
    values = jax.random.normal(third, (N_GRP, D, OUTW), jnp.float32)
    return values * rows[None, :, None] * cols[None, None, :]


def draw_block_counts(key, part):
    first, second = jax.random.split(jax.random.fold_in(key, 53))
    hot_count = max(1, N_DEV // 8)
    offset = jax.random.randint(first, (N_GRP, 1), 0, N_DEV)
    hot = (jnp.arange(N_DEV, dtype=jnp.int32)[None, :] - offset) % N_DEV < hot_count
    other = jax.random.randint(second, (N_GRP, N_DEV, N_DEV), 0, CAP // 2 + 1)
    return jnp.where(hot[:, None, :], CAP, other).astype(jnp.int32)


def with_ends(values, key, low, largest):
    place = [jax.random.randint(jax.random.fold_in(key, axis), (), 0, length) for axis, length in enumerate(values.shape)]
    main_axis = values.shape.index(max(values.shape))
    beside = place[:main_axis] + [(place[main_axis] + 1) % values.shape[main_axis]] + place[main_axis + 1:]
    return values.at[tuple(place)].set(low).at[tuple(beside)].set(largest)


def shard_levels(key, shape, shards, least, high):
    level, own = 1.0, jax.random.fold_in(key, 6)
    for position, blocks in shards:
        heights = jnp.exp(jax.random.uniform(jax.random.fold_in(own, position), (blocks,), jnp.float32, least / len(shards), high / len(shards)))
        level = level * jnp.repeat(heights, shape[position] // blocks).reshape([-1 if axis == position else 1 for axis in range(len(shape))])
    return level


def gaussian(stream_key, extent, scale, limit, pieces=(), kind=jnp.bfloat16):
    values = scale * jax.random.normal(stream_key, extent, jnp.float32)
    if pieces:
        values = values * shard_levels(stream_key, extent, pieces, -0.22, 0.18)
    return jnp.clip(values, -limit, limit).astype(kind)


def setup_inputs(seed: int = 0) -> dict:
    seeds = jax.random.split(jax.random.key(seed), 10)
    layer_inputs = draw_layer_inputs(jax.random.fold_in(seeds[9], 71), 0)
    output_grads = draw_output_grads(jax.random.fold_in(seeds[9], 71), 0)
    layer_owner = jax.random.permutation(seeds[2], LAYERS).astype(jnp.int32)
    master_weights = draw_master_weights(jax.random.fold_in(seeds[9], 71), 0)
    momentum = gaussian(seeds[4], (N_GRP, D, OUTW), 1.0, 6.0, ((0, 8), (1, 32)), jnp.float32)
    table_blocks = gaussian(seeds[5], (N_GRP, N_DEV * NB, BLK, E), 1.0, 6.0, ((0, 8), (1, 32)), jnp.float32)
    block_grads = gaussian(seeds[6], (N_GRP, N_DEV, N_DEV * CAP, BLK, E), 1.0, 6.0, ((0, 8), (1, 32)))
    block_ids = with_ends(jax.random.randint(seeds[7], (N_GRP, N_DEV, N_DEV * CAP), 0, NB), jax.random.fold_in(seeds[7], 1), 0, NB - 1).astype(jnp.int32)
    block_counts = draw_block_counts(jax.random.fold_in(seeds[9], 71), 0)
    return {"layer_inputs": layer_inputs, "output_grads": output_grads, "layer_owner": layer_owner, "master_weights": master_weights, "momentum": momentum, "table_blocks": table_blocks, "block_grads": block_grads, "block_ids": block_ids, "block_counts": block_counts}


tower_rate = 0.5
momentum_keep = 0.9
tower_decay = 0.1
table_rate = 0.5
table_decay = 0.2
eps_norm = 1e-06

def reference(layer_inputs, output_grads, layer_owner, master_weights, momentum, table_blocks, block_grads, block_ids, block_counts):
    slot_layer = jnp.argsort(layer_owner).astype(jnp.int32)

    def layer_grad(index):
        inputs = layer_inputs[index].astype(jnp.float32)
        cotangent = output_grads[index].astype(jnp.float32)
        return jnp.dot(inputs.T, cotangent, precision=lax.Precision.HIGHEST)
    grad = lax.map(layer_grad, slot_layer)
    weight_sq = lax.optimization_barrier(jnp.sum(master_weights * master_weights, axis=(1, 2)))
    grad_sq = lax.optimization_barrier(jnp.sum(grad * grad, axis=(1, 2)))
    weight_norm = jnp.sqrt(weight_sq + eps_norm)
    trust = weight_norm / (jnp.sqrt(grad_sq + eps_norm) + tower_decay * weight_norm)
    new_momentum = momentum_keep * momentum + tower_rate * trust[:, None, None] * (grad + tower_decay * master_weights)
    new_master = master_weights - new_momentum
    new_weights = new_master[layer_owner.astype(jnp.int32)].astype(jnp.bfloat16)
    ndev = block_counts.shape[1]
    cap = block_ids.shape[2] // ndev
    nblocks = table_blocks.shape[1]
    width = table_blocks.shape[2] * table_blocks.shape[3]
    slot_index = jnp.arange(ndev * cap, dtype=jnp.int32)
    owner_of_slot = slot_index // cap

    def group_update(items):
        grads_g, ids_g, counts_g, table_g = items
        live = (slot_index % cap)[None, :] < jnp.repeat(counts_g, cap, axis=1)
        target = owner_of_slot[None, :] * (nblocks // ndev) + ids_g
        target = jnp.where(live, target, nblocks).reshape(-1)
        data = grads_g.reshape(ndev * ndev * cap, width).astype(jnp.float32)
        sums = jax.ops.segment_sum(data, target, num_segments=nblocks + 1)[:nblocks]
        hits = jax.ops.segment_sum(live.reshape(-1).astype(jnp.int32), target, num_segments=nblocks + 1)[:nblocks]
        flat = table_g.reshape(nblocks, width)
        w_norm = jnp.sqrt(lax.optimization_barrier(jnp.sum(flat * flat, axis=1)) + eps_norm)
        g_norm = jnp.sqrt(lax.optimization_barrier(jnp.sum(sums * sums, axis=1)) + eps_norm)
        block_trust = w_norm / (g_norm + table_decay * w_norm)
        moved = flat - table_rate * block_trust[:, None] * (sums + table_decay * flat)
        return jnp.where((hits > 0)[:, None], moved, flat).reshape(table_g.shape)
    new_table = lax.map(group_update, (block_grads, block_ids, block_counts, table_blocks))
    return (new_master, new_momentum, new_weights, new_table)
```

```python
import functools

import jax
import jax.numpy as jnp
from jax import lax
from jax.experimental import pallas as pl
from jax.experimental.pallas import tpu as pltpu
from jax.sharding import PartitionSpec as P

tower_rate = 0.5
momentum_keep = 0.9
tower_decay = 0.1
table_rate = 0.5
table_decay = 0.2
eps_norm = 1e-06

NZ = 8
NX = 4
NY = 4
ND = NX * NY * 2
NCHIP = NX * NY


def step_kernel(
    owner,
    ids,
    counts,
    x_hbm,
    g_hbm,
    w_hbm,
    m_hbm,
    t_hbm,
    bg_hbm,
    slots_out,
    w_out,
    m_out,
    t_out,
    x_in,
    x_slot,
    x_all,
    x_turn,
    g_in,
    g_slot,
    g_all,
    acc,
    grad,
    w,
    m,
    table,
    sums,
    got,
    tag,
    got_tag,
    norms,
    slabs,
    in_sem,
    out_sem,
    gz_send,
    gz_recv,
    xz_send,
    xz_recv,
    xp_send,
    xp_recv,
    ag_send,
    r1,
    r2,
    r3,
    r4,
    half_send,
    half_recv,
    norm_send,
    norm_recv,
    bg_send,
    bg_recv,
    tag_send,
    tag_recv,
    own_sem,
    wz_send,
    wz_recv,
    slab_sem,
):
    z = lax.axis_index("grp")
    d = lax.axis_index("dev")
    core = d % 2
    cx = (d // 2) % NX
    cy = d // (2 * NX)
    chip = d // 2
    pal = chip * 2 + 1 - core
    rows = w_hbm.shape[1]
    cols = w_hbm.shape[2]
    half = cols // 2
    per = g_hbm.shape[1]
    pair = 2 * per
    tokens = x_hbm.shape[1]

    def spot(a, b):
        sx = (cx + a * (1 - core) + b * core + NX) % NX
        sy = (cy + a * core + b * (1 - core) + NY) % NY
        return sy * NX + sx

    def send(src, dst, s_sem, r_sem, zz, dd):
        pltpu.make_async_remote_copy(
            src_ref=src,
            dst_ref=dst,
            send_sem=s_sem,
            recv_sem=r_sem,
            device_id=(zz, dd),
            device_id_type=pl.DeviceIdType.MESH,
        ).start()

    def arrived(ref, sem):
        pltpu.make_async_copy(ref, ref, sem).wait()

    def column(i):
        off = (i % 2) * ((i + 1) // 2) + (1 - i % 2) * (NZ - i // 2)
        return (z + off) % NZ

    x_load = pltpu.make_async_copy(x_hbm, x_in, in_sem.at[0])
    g_load = pltpu.make_async_copy(g_hbm, g_in, in_sem.at[1])
    g_load.start()
    x_load.start()
    w_load = pltpu.make_async_copy(w_hbm.at[0], w, in_sem.at[2])
    m_load = pltpu.make_async_copy(m_hbm.at[0], m, in_sem.at[3])
    t_load = pltpu.make_async_copy(t_hbm.at[0], table, in_sem.at[4])
    own_load = pltpu.make_async_copy(
        bg_hbm.at[0, 0, pl.ds(2 * d, 2)], got.at[pl.ds(2 * d, 2)], own_sem
    )
    w_load.start()
    m_load.start()
    t_load.start()
    own_load.start()

    barrier = pltpu.get_barrier_semaphore()

    @pl.loop(1, ND)
    def _(p):
        pl.semaphore_signal(
            barrier, inc=1, device_id=(z, (d + p) % ND), device_id_type=pl.DeviceIdType.MESH
        )

    @pl.loop(1, NZ)
    def _(p):
        for cc in range(2):
            pl.semaphore_signal(
                barrier,
                inc=1,
                device_id=((z + p) % NZ, chip * 2 + cc),
                device_id_type=pl.DeviceIdType.MESH,
            )

    def layer_of(s):
        found = jnp.int32(0)
        for l in range(NZ):
            found = jnp.where(owner[l] == s, l, found)
        return found

    g_load.wait()

    @pl.loop(0, NZ)
    def _(s):
        l = layer_of(s)
        for h in range(2):
            g_slot[h, s] = g_in[l, :, h * half : (h + 1) * half]

    g_all[z, chip, pl.ds(core * per, per), :] = g_slot[core, z]
    x_load.wait()

    @pl.loop(0, NZ)
    def _(s):
        l = layer_of(s)
        x_slot[s] = x_in[l]

    x_all[z, core] = x_slot[z]

    pl.semaphore_wait(barrier, ND - 1 + 2 * (NZ - 1))

    send(
        g_slot.at[1 - core, z],
        g_all.at[z, chip, pl.ds(core * per, per)],
        gz_send.at[1],
        gz_recv.at[z, core],
        z,
        pal,
    )

    @pl.loop(1, NZ)
    def _(i):
        zt = column(i)
        for cc in range(2):
            send(
                g_slot.at[cc, zt],
                g_all.at[z, chip, pl.ds(core * per, per)],
                gz_send.at[0],
                gz_recv.at[z, core],
                zt,
                chip * 2 + cc,
            )

    send(x_all.at[z, core], x_all.at[z, core], xp_send, xp_recv.at[z], z, pal)

    @pl.loop(1, NZ)
    def _(i):
        zt = column(i)
        send(x_slot.at[zt], x_all.at[z, core], xz_send, xz_recv.at[z], zt, d)

    @pl.loop(0, ND)
    def _(j):
        for r in range(2):
            t = jnp.where(r < counts[0, 0, j], ids[0, 0, 2 * j + r], -1)
            tag[j, r : r + 1, :] = jnp.full((1, tag.shape[2]), t, jnp.int32)

    got_tag[d] = tag[d]
    acc[...] = jnp.zeros_like(acc)
    w_load.wait()
    weight_sq = jnp.zeros((8, 128), jnp.float32)

    def weight_step(i, total):
        v = w[pl.ds(pl.multiple_of(i * 8, 8), 8), :]
        v = v * v
        for k in range(cols // 128):
            total = total + v[:, k * 128 : (k + 1) * 128]
        return total

    weight_sq = lax.fori_loop(0, rows // 8, weight_step, weight_sq)

    def dev_at(a, b):
        return spot(a, b) * 2 + core

    steps = (0, -1, 1, 2)

    def piece(zc, k):
        return g_all.at[zc, k]

    def part(zc, k, h):
        return g_all.at[zc, k, pl.ds(h * per, per)]

    def spread(zc, q):
        k = spot(steps[q], 0)
        send(piece(zc, k), piece(zc, k), ag_send.at[zc], r3.at[zc, q, 0], z, dev_at(0, 1))
        send(piece(zc, k), piece(zc, k), ag_send.at[zc], r3.at[zc, q, 1], z, dev_at(0, -1))

    @pl.loop(0, NZ + 6)
    def _(it):
        @pl.when(it < NZ)
        def _():
            zc = column(it)

            @pl.when(it == 0)
            def _():
                arrived(
                    g_all.at[zc, chip, pl.ds((1 - core) * per, per)], gz_recv.at[zc, 1 - core]
                )

            @pl.when(it > 0)
            def _():
                for cc in range(2):
                    arrived(g_all.at[zc, chip, pl.ds(cc * per, per)], gz_recv.at[zc, cc])

            send(piece(zc, chip), piece(zc, chip), ag_send.at[zc], r1.at[zc, 0], z, dev_at(1, 0))
            send(piece(zc, chip), piece(zc, chip), ag_send.at[zc], r1.at[zc, 1], z, dev_at(-1, 0))
            spread(zc, 0)

        @pl.when((it >= 1) & (it < NZ + 1))
        def _():
            zc = column(it - 1)
            k = spot(-1, 0)
            arrived(piece(zc, k), r1.at[zc, 0])
            send(part(zc, k, 0), part(zc, k, 0), ag_send.at[zc], r2.at[zc, 0], z, dev_at(1, 0))
            spread(zc, 1)
            k = spot(1, 0)
            arrived(piece(zc, k), r1.at[zc, 1])
            send(part(zc, k, 1), part(zc, k, 1), ag_send.at[zc], r2.at[zc, 1], z, dev_at(-1, 0))
            spread(zc, 2)

        @pl.when((it >= 2) & (it < NZ + 2))
        def _():
            zc = column(it - 2)
            k = spot(2, 0)
            for h in range(2):
                arrived(part(zc, k, h), r2.at[zc, h])
            spread(zc, 3)

        @pl.when((it >= 3) & (it < NZ + 3))
        def _():
            zc = column(it - 3)
            for q in range(4):
                k = spot(steps[q], -1)
                arrived(piece(zc, k), r3.at[zc, q, 0])
                send(part(zc, k, 0), part(zc, k, 0), ag_send.at[zc], r4.at[zc, q, 0], z, dev_at(0, 1))
                k = spot(steps[q], 1)
                arrived(piece(zc, k), r3.at[zc, q, 1])
                send(part(zc, k, 1), part(zc, k, 1), ag_send.at[zc], r4.at[zc, q, 1], z, dev_at(0, -1))

        @pl.when((it >= 4) & (it < NZ + 4))
        def _():
            zc = column(it - 4)
            for q in range(4):
                k = spot(steps[q], 2)
                for h in range(2):
                    arrived(part(zc, k, h), r4.at[zc, q, h])

            @pl.when(it > 4)
            def _():
                arrived(x_all.at[zc, core], xz_recv.at[zc])
                send(x_all.at[zc, core], x_all.at[zc, core], xp_send, xp_recv.at[zc], z, pal)

        @pl.when(it >= 6)
        def _():
            zc = column(it - 6)
            arrived(x_all.at[zc, 1 - core], xp_recv.at[zc])
            for cc in range(2):
                x_turn[cc * rows : (cc + 1) * rows, :] = x_all[zc, cc].T

            @pl.loop(0, half // 256)
            def _(n):
                where = pl.ds(pl.multiple_of(n * 256, 256), 256)
                block = g_all[zc, :, :, where].reshape(tokens, 256)
                acc[:, where] += jnp.dot(
                    x_turn[...], block, preferred_element_type=jnp.float32
                )

    send(
        acc.at[pl.ds((1 - core) * rows, rows)],
        grad.at[:, pl.ds(core * half, half)],
        half_send,
        half_recv,
        z,
        pal,
    )

    def grad_step(i, total):
        v = acc[pl.ds(pl.multiple_of(i * 8, 8), 8), :]
        v = v * v
        for k in range(half // 128):
            total = total + v[:, k * 128 : (k + 1) * 128]
        return total

    grad_sq = lax.fori_loop(0, 2 * rows // 8, grad_step, jnp.zeros((8, 128), jnp.float32))
    norms[d, 0] = weight_sq
    norms[d, 1] = grad_sq

    @pl.loop(1, ND)
    def _(p):
        send(norms.at[d], norms.at[d], norm_send, norm_recv.at[d], z, (d + p) % ND)

    grad[:, pl.ds(core * half, half)] = acc[pl.ds(core * rows, rows), :]
    m_load.wait()

    @pl.loop(1, ND)
    def _(p):
        j = (d + p) % ND
        arrived(norms.at[j], norm_recv.at[j])

    totals = jnp.sum(norms[...], axis=0)
    weight_total = jnp.sum(totals[0], keepdims=True)
    grad_total = jnp.sum(totals[1], keepdims=True)
    weight_norm = jnp.sqrt(weight_total + eps_norm)
    trust = weight_norm / (jnp.sqrt(grad_total + eps_norm) + tower_decay * weight_norm)
    scale = tower_rate * trust
    arrived(grad.at[:, pl.ds((1 - core) * half, half)], half_recv)

    strip = 16
    cut = rows // 2

    def slab(s, h):
        return slabs.at[s, pl.ds(h * cut, cut)]

    for h in range(2):

        @pl.loop(0, cut // strip)
        def _(i):
            at = pl.ds(pl.multiple_of(h * cut + i * strip, strip), strip)
            old = w[at, :]
            new_m = momentum_keep * m[at, :] + scale * (grad[at, :] + tower_decay * old)
            new_w = old - new_m
            m[at, :] = new_m
            w[at, :] = new_w
            slabs[z, at, :] = new_w.astype(jnp.bfloat16)

        send(slab(z, h), slab(z, h), wz_send, wz_recv.at[0, 0, h], (z + 1) % NZ, d)
        send(slab(z, h), slab(z, h), wz_send, wz_recv.at[1, 0, h], (z + NZ - 1) % NZ, d)

    @pl.loop(1, ND)
    def _(p):
        j = (d + p) % ND
        send(
            bg_hbm.at[0, 0, pl.ds(2 * j, 2)],
            got.at[pl.ds(2 * d, 2)],
            bg_send,
            bg_recv.at[d],
            z,
            j,
        )
        send(tag.at[j], got_tag.at[d], tag_send, tag_recv.at[d], z, j)

    w_store = pltpu.make_async_copy(w, w_out.at[0], out_sem.at[0])
    m_store = pltpu.make_async_copy(m, m_out.at[0], out_sem.at[1])
    w_store.start()
    m_store.start()
    pltpu.make_async_copy(slabs.at[z], slots_out.at[z], slab_sem).start()

    for j in range(1, 4):
        low = (z + NZ - j) % NZ
        high = (z + j) % NZ
        for h in range(2):
            arrived(slab(low, h), wz_recv.at[0, j - 1, h])
            if j < 3 or h == 0:
                send(slab(low, h), slab(low, h), wz_send, wz_recv.at[0, j, h], (z + 1) % NZ, d)
            arrived(slab(high, h), wz_recv.at[1, j - 1, h])
            if j < 3 or h == 1:
                send(slab(high, h), slab(high, h), wz_send, wz_recv.at[1, j, h], (z + NZ - 1) % NZ, d)
        pltpu.make_async_copy(slabs.at[low], slots_out.at[low], slab_sem).start()
        pltpu.make_async_copy(slabs.at[high], slots_out.at[high], slab_sem).start()

    own_load.wait()
    t_load.wait()

    @pl.loop(1, ND)
    def _(p):
        j = (d + p) % ND
        arrived(got.at[pl.ds(2 * j, 2)], bg_recv.at[j])
        arrived(got_tag.at[j], tag_recv.at[j])

    nb = table.shape[0]
    wide = table.shape[2]

    @pl.loop(0, table.shape[1] // strip)
    def _(i):
        at = pl.ds(pl.multiple_of(i * strip, strip), strip)

        def add(s, totals):
            totals = list(totals)
            for r in range(2):
                name = got_tag[s, r : r + 1, :]
                value = got[2 * s + r, at, :].astype(jnp.float32)
                for b in range(nb):
                    totals[b] = totals[b] + jnp.where(name == b, value, 0.0)
            return tuple(totals)

        totals = lax.fori_loop(
            0, ND, add, tuple(jnp.zeros((strip, wide), jnp.float32) for _ in range(nb))
        )
        for b in range(nb):
            sums[b, at, :] = totals[b]

    names = got_tag[:, 0:2, :]
    for b in range(nb):
        hits = jnp.sum(jnp.where(names == b, 1.0, 0.0), axis=(0, 1)).reshape(1, wide)
        flat = table[b]
        total = sums[b]
        w_norm = jnp.sqrt(jnp.sum(flat * flat, keepdims=True) + eps_norm)
        g_norm = jnp.sqrt(jnp.sum(total * total, keepdims=True) + eps_norm)
        block_trust = w_norm / (g_norm + table_decay * w_norm)
        moved = flat - table_rate * block_trust * (total + table_decay * flat)
        table[b] = jnp.where(hits > 0, moved, flat)
    t_store = pltpu.make_async_copy(table, t_out.at[0], out_sem.at[2])
    t_store.start()

    far = (z + 4) % NZ
    arrived(slab(far, 0), wz_recv.at[0, 3, 0])
    arrived(slab(far, 1), wz_recv.at[1, 3, 1])
    pltpu.make_async_copy(slabs.at[far], slots_out.at[far], slab_sem).start()

    arrived(g_slot.at[0, 0], gz_send.at[1])
    arrived(g_slot.at[:, 0:7], gz_send.at[0])
    arrived(x_slot.at[0:7], xz_send)
    arrived(x_slot, xp_send)

    @pl.loop(0, NZ)
    def _(k):
        arrived(g_all.at[k, 0 : NCHIP - 1], ag_send.at[k])

    arrived(acc.at[0:rows], half_send)
    arrived(norms.at[0 : ND - 1], norm_send)
    arrived(got.at[0 : 2 * (ND - 1)], bg_send)
    arrived(tag.at[0 : ND - 1], tag_send)
    arrived(slabs.at[0:7], wz_send)
    w_store.wait()
    m_store.wait()
    t_store.wait()
    pltpu.make_async_copy(slabs, slots_out, slab_sem).wait()


def finish_kernel(owner, slots, new_w, new_m, new_t, out, w_out, m_out, t_out):
    out[...] = slots[...]
    w_out[...] = new_w[...]
    m_out[...] = new_m[...]
    t_out[...] = new_t[...]


def local(
    layer_inputs,
    output_grads,
    layer_owner,
    master_weights,
    momentum,
    table_blocks,
    block_grads,
    block_ids,
    block_counts,
):
    layers, tokens, rows = layer_inputs.shape
    per, cols = output_grads.shape[1:]
    half = cols // 2
    nb, tall, wide = table_blocks.shape[1:]
    f32, bf16, i32 = jnp.float32, jnp.bfloat16, jnp.int32
    hbm = pl.BlockSpec(memory_space=pltpu.HBM)
    smem = pl.BlockSpec(memory_space=pltpu.SMEM)
    dma = pltpu.SemaphoreType.DMA
    slots, new_w, new_m, new_t = pl.pallas_call(
        step_kernel,
        name="step",
        out_shape=(
            jax.ShapeDtypeStruct((NZ, rows, cols), bf16),
            jax.ShapeDtypeStruct(master_weights.shape, f32),
            jax.ShapeDtypeStruct(momentum.shape, f32),
            jax.ShapeDtypeStruct(table_blocks.shape, f32),
        ),
        in_specs=[smem, smem, smem] + [hbm] * 6,
        out_specs=(hbm, hbm, hbm, hbm),
        scratch_shapes=[
            pltpu.VMEM((layers, tokens, rows), bf16),
            pltpu.VMEM((layers, tokens, rows), bf16),
            pltpu.VMEM((NZ, 2, tokens, rows), bf16),
            pltpu.VMEM((2 * rows, tokens), bf16),
            pltpu.VMEM((layers, per, cols), bf16),
            pltpu.VMEM((2, layers, per, half), bf16),
            pltpu.VMEM((NZ, NCHIP, 2 * per, half), bf16),
            pltpu.VMEM((2 * rows, half), f32),
            pltpu.VMEM((rows, cols), f32),
            pltpu.VMEM((rows, cols), f32),
            pltpu.VMEM((rows, cols), f32),
            pltpu.VMEM((nb, tall, wide), f32),
            pltpu.VMEM((nb, tall, wide), f32),
            pltpu.VMEM((2 * ND, tall, wide), bf16),
            pltpu.VMEM((ND, 8, wide), i32),
            pltpu.VMEM((ND, 8, wide), i32),
            pltpu.VMEM((ND, 2, 8, 128), f32),
            pltpu.VMEM((NZ, rows, cols), bf16),
            dma((5,)),
            dma((3,)),
            dma((2,)),
            dma((NZ, 2)),
            dma,
            dma((NZ,)),
            dma,
            dma((NZ,)),
            dma((NZ,)),
            dma((NZ, 2)),
            dma((NZ, 2)),
            dma((NZ, 4, 2)),
            dma((NZ, 4, 2)),
            dma,
            dma,
            dma,
            dma((ND,)),
            dma,
            dma((ND,)),
            dma,
            dma((ND,)),
            dma,
            dma,
            dma((2, 4, 2)),
            dma,
        ],
        compiler_params=pltpu.CompilerParams(
            collective_id=0, has_side_effects=True, vmem_limit_bytes=60 * 1024 * 1024
        ),
    )(
        layer_owner,
        block_ids,
        block_counts,
        layer_inputs,
        output_grads,
        master_weights,
        momentum,
        table_blocks,
        block_grads,
    )
    share = rows // layers
    by_rows = pl.BlockSpec((1, share, cols), lambda l, owner: (0, l, 0))
    by_block = pl.BlockSpec((1, nb // layers, tall, wide), lambda l, owner: (0, l, 0, 0))
    new_weights, new_master, new_moment, new_table = pl.pallas_call(
        finish_kernel,
        name="finish",
        grid_spec=pltpu.PrefetchScalarGridSpec(
            num_scalar_prefetch=1,
            grid=(layers,),
            in_specs=[
                pl.BlockSpec((1, rows, cols), lambda l, owner: (owner[l], 0, 0)),
                by_rows,
                by_rows,
                by_block,
            ],
            out_specs=[
                pl.BlockSpec((1, rows, cols), lambda l, owner: (l, 0, 0)),
                by_rows,
                by_rows,
                by_block,
            ],
        ),
        out_shape=(
            jax.ShapeDtypeStruct((layers, rows, cols), bf16),
            jax.ShapeDtypeStruct(master_weights.shape, f32),
            jax.ShapeDtypeStruct(momentum.shape, f32),
            jax.ShapeDtypeStruct(table_blocks.shape, f32),
        ),
    )(layer_owner, slots, new_w, new_m, new_t)
    return new_master, new_moment, new_weights, new_table


def solution(mesh):
    return jax.shard_map(
        local,
        mesh=mesh,
        in_specs=(
            P(None, "grp", "dev"),
            P(None, ("grp", "dev"), None),
            P(),
            P("grp", "dev", None),
            P("grp", "dev", None),
            P("grp", "dev", None, None),
            P("grp", "dev", None, None, None),
            P("grp", "dev", None),
            P("grp", "dev", None),
        ),
        out_specs=(
            P("grp", "dev", None),
            P("grp", "dev", None),
            P(None, "dev", None),
            P("grp", "dev", None, None),
        ),
        check_vma=False,
    )
```

```python
import functools

import jax
import jax.numpy as jnp
from jax import lax
from jax.experimental import pallas as pl
from jax.experimental.pallas import tpu as pltpu
from jax.sharding import PartitionSpec as P

tower_rate = 0.5
momentum_keep = 0.9
tower_decay = 0.1
table_rate = 0.5
table_decay = 0.2
eps_norm = 1e-06

NZ = 8
NX = 4
NY = 4
ND = NX * NY * 2


def step_kernel(
    owner,
    ids,
    counts,
    x_hbm,
    g_hbm,
    w_hbm,
    m_hbm,
    t_hbm,
    bg_hbm,
    slabs,
    w,
    m,
    table,
    x_in,
    x_slot,
    x_all,
    x_turn,
    x_relay,
    g_in,
    g_slot,
    g_all,
    g_relay,
    acc,
    grad,
    sums,
    pick,
    turned,
    got,
    tag,
    got_tag,
    norms,
    in_sem,
    gz_send,
    gz_recv,
    go_send,
    gr_send,
    gr_recv,
    gf_send,
    xz_send,
    xz_recv,
    xr_send,
    xr_recv,
    xf_send,
    xo_send,
    xo_recv,
    xp_send,
    xp_recv,
    ag_send,
    ag_recv,
    half_send,
    half_recv,
    norm_send,
    norm_recv,
    bg_send,
    bg_recv,
    tag_send,
    tag_recv,
    wz_send,
    wz_recv,
):
    z = lax.axis_index("grp")
    d = lax.axis_index("dev")
    core = d % 2
    cx = (d // 2) % NX
    cy = d // (2 * NX)
    chip = d // 2
    side = cy // 2
    duo = ((cy + 1) // 2) % 2
    oy = NY - 1 - cy
    iy = cy + 1 - 2 * (cy % 2)
    me = side * 2 + core
    pal = chip * 2 + 1 - core
    outer = (oy * NX + cx) * 2 + core
    inner = (iy * NX + cx) * 2 + core
    right = (cy * NX + (cx + 1) % NX) * 2 + core
    left = (cy * NX + (cx + NX - 1) % NX) * 2 + core
    rows = w_hbm.shape[1]
    cols = w_hbm.shape[2]
    quarter = cols // 4
    per = g_hbm.shape[1]
    tokens = x_hbm.shape[1]
    band = tokens // NY

    def send(src, dst, s_sem, r_sem, zz, dd):
        pltpu.make_async_remote_copy(
            src_ref=src,
            dst_ref=dst,
            send_sem=s_sem,
            recv_sem=r_sem,
            device_id=(zz, dd),
            device_id_type=pl.DeviceIdType.MESH,
        ).start()

    def arrived(ref, sem):
        pltpu.make_async_copy(ref, ref, sem).wait()

    def column(i):
        off = (i % 2) * ((i + 1) // 2) + (1 - i % 2) * (NZ - i // 2)
        return (z + off) % NZ

    def holder(p, cc):
        y = jnp.where(p == side, cy, oy)
        return (y * NX + cx) * 2 + cc

    g_load = pltpu.make_async_copy(g_hbm, g_in, in_sem.at[1])
    x_load = pltpu.make_async_copy(x_hbm, x_in, in_sem.at[0])
    w_load = pltpu.make_async_copy(w_hbm.at[0], w.at[0], in_sem.at[2])
    m_load = pltpu.make_async_copy(m_hbm.at[0], m.at[0], in_sem.at[3])
    t_load = pltpu.make_async_copy(t_hbm.at[0], table.at[0], in_sem.at[4])
    own_load = pltpu.make_async_copy(
        bg_hbm.at[0, 0, pl.ds(2 * d, 2)], got.at[pl.ds(2 * d, 2)], in_sem.at[5]
    )
    g_load.start()
    x_load.start()
    w_load.start()
    m_load.start()
    t_load.start()
    own_load.start()

    barrier = pltpu.get_barrier_semaphore()

    @pl.loop(1, ND)
    def _(p):
        pl.semaphore_signal(
            barrier, inc=1, device_id=(z, (d + p) % ND), device_id_type=pl.DeviceIdType.MESH
        )

    @pl.loop(1, NZ)
    def _(p):
        for ps in range(2):
            for cc in range(2):
                pl.semaphore_signal(
                    barrier,
                    inc=1,
                    device_id=((z + p) % NZ, holder(ps, cc)),
                    device_id_type=pl.DeviceIdType.MESH,
                )

    def layer_of(s):
        found = jnp.int32(0)
        for l in range(NZ):
            found = jnp.where(owner[l] == s, l, found)
        return found
    g_load.wait()

    @pl.loop(0, NZ)
    def _(s):
        l = layer_of(s)
        for q in range(4):
            g_slot[s, q] = g_in[l, :, q * quarter : (q + 1) * quarter]

    g_all[z, duo, side, cx, pl.ds(core * per, per), :] = g_slot[z, me]
    x_load.wait()

    @pl.loop(0, NZ)
    def _(s):
        l = layer_of(s)
        x_slot[s] = x_in[l]

    x_all[z, me] = x_slot[z]
    pl.semaphore_wait(barrier, ND - 1 + 4 * (NZ - 1))
    def g_home(zs):
        return g_all.at[zs, duo, side, cx, pl.ds(core * per, per)]

    far = (z + NZ // 2) % NZ
    ways = (1, NZ - 1)
    deep = tokens // 2
    for way in range(2):
        zn = (z + ways[way]) % NZ
        send(g_slot.at[far, 2 * way : 2 * way + 2], g_relay.at[way], gr_send, gr_recv.at[way], zn, d)
        send(
            x_slot.at[far, way * deep : (way + 1) * deep],
            x_relay.at[way],
            xr_send,
            xr_recv.at[way],
            zn,
            d,
        )
    send(g_slot.at[z, side * 2 + 1 - core], g_home(z), go_send.at[0], gz_recv.at[z, me], z, pal)
    for cc in range(2):
        send(
            g_slot.at[z, (1 - side) * 2 + cc],
            g_home(z),
            go_send.at[1 + cc],
            gz_recv.at[z, me],
            z,
            (oy * NX + cx) * 2 + cc,
        )

    def g_out(i):
        zt = column(i)
        for ps in range(2):
            for cc in range(2):
                send(
                    g_slot.at[zt, 2 * ps + cc],
                    g_home(z),
                    gz_send,
                    gz_recv.at[z, me],
                    zt,
                    holder(ps, cc),
                )

    def x_out(i):
        zt = column(i)
        send(x_slot.at[zt], x_all.at[z, me], xz_send, xz_recv.at[z, 0], zt, d)

    def x_share(ref, zs, h):
        send(ref, ref, xo_send, xo_recv.at[zs, h], z, outer)
        send(ref, ref, xp_send, xp_recv.at[zs, 0, h], z, pal)

    def x_half(zs, s, h):
        return x_all.at[zs, s, pl.ds(h * deep, deep)]

    @pl.loop(1, 5)
    def _(i):
        g_out(i)

    @pl.loop(1, 3)
    def _(i):
        x_out(i)

    @pl.loop(5, 7)
    def _(i):
        g_out(i)

    @pl.loop(3, 5)
    def _(i):
        x_out(i)

    x_share(x_all.at[z, me], z, 0)

    def whole(zs, pr, da):
        return g_all.at[zs, pr, :, (cx + da + NX) % NX]

    def part(zs, pr, da, h):
        return g_all.at[zs, pr, h, (cx + da + NX) % NX]

    def push(ref, zs, k, dd):
        send(ref, ref, ag_send, ag_recv.at[zs, k], z, dd)

    def landed(it):
        zs = column(it)

        @pl.when(it == 0)
        def _():
            for j, who in enumerate((pal, (oy * NX + cx) * 2, (oy * NX + cx) * 2 + 1)):
                wy = who // (2 * NX)
                wc = who % 2
                arrived(
                    g_all.at[z, duo, wy // 2, cx, pl.ds(wc * per, per)],
                    gz_recv.at[z, (wy // 2) * 2 + wc],
                )

        @pl.when(it > 0)
        def _():
            for ps in range(2):
                for cc in range(2):
                    arrived(
                        g_all.at[zs, duo, ps, cx, pl.ds(cc * per, per)],
                        gz_recv.at[zs, 2 * ps + cc],
                    )

    def relay():
        for way in range(2):
            zs = (z + NZ - ways[way]) % NZ
            zt = (zs + NZ // 2) % NZ
            arrived(g_relay.at[way], gr_recv.at[way])
            for cc in range(2):
                send(
                    g_relay.at[way, cc], g_home(zs), gf_send, gz_recv.at[zs, me], zt, holder(way, cc)
                )

        @pl.loop(5, 7)
        def _(i):
            x_out(i)

        for way in range(2):
            zs = (z + NZ - ways[way]) % NZ
            zt = (zs + NZ // 2) % NZ
            arrived(x_relay.at[way], xr_recv.at[way])
            send(
                x_relay.at[way],
                x_all.at[zs, me, pl.ds(way * deep, deep)],
                xf_send,
                xz_recv.at[zs, way],
                zt,
                d,
            )

    there = (1 - side) * 2 + core

    def x_stages(it):
        lag = jnp.where(it < NZ, 0, 2)

        @pl.when(((it >= 3) & (it < 7)) | ((it >= 9) & (it < 11)))
        def _():
            zs = column(it - 2 - lag)
            arrived(x_all.at[zs, me], xz_recv.at[zs, 0])
            x_share(x_all.at[zs, me], zs, 0)

        @pl.when(it == 11)
        def _():
            zs = column(NZ - 1)
            for h in range(2):
                arrived(x_half(zs, me, h), xz_recv.at[zs, h])
                x_share(x_half(zs, me, h), zs, h)

        lead = jnp.where(it < 9, 0, 2)

        @pl.when(((it >= 4) & (it < 9)) | (it >= 11))
        def _():
            zs = column(it - 4 - lead)

            @pl.when(it < NZ + 5)
            def _():
                for sd in range(2):
                    arrived(
                        x_all.at[zs, sd * 2 + 1 - core],
                        xp_recv.at[zs, jnp.where(sd == side, 0, 1), 0],
                    )

            @pl.when(it == NZ + 5)
            def _():
                for h in range(2):
                    for sd in range(2):
                        arrived(
                            x_half(zs, sd * 2 + 1 - core, h),
                            xp_recv.at[zs, jnp.where(sd == side, 0, 1), h],
                        )
            @pl.loop(0, 4)
            def _(s):
                for y in range(NY):
                    order = ((y + 1) // 2) % 2 * 2 + y // 2
                    x_turn[pl.ds(s * rows, rows), order * band : (order + 1) * band] = x_all[
                        zs, s, y * band : (y + 1) * band, :
                    ].T

            @pl.loop(0, quarter // 256)
            def _(n):
                where = pl.ds(pl.multiple_of(n * 256, 256), 256)
                block = g_all[zs, :, :, :, :, where].reshape(tokens, 256)
                acc[:, where] += jnp.dot(x_turn[...], block, preferred_element_type=jnp.float32)

        @pl.when(((it >= 3) & (it < 8)) | ((it >= 10) & (it < 12)))
        def _():
            zs = column(it - 3 - jnp.where(it < 8, 0, 2))
            arrived(x_all.at[zs, there], xo_recv.at[zs, 0])
            send(x_all.at[zs, there], x_all.at[zs, there], xp_send, xp_recv.at[zs, 1, 0], z, pal)

        @pl.when(it == 12)
        def _():
            zs = column(NZ - 1)
            for h in range(2):
                arrived(x_half(zs, there, h), xo_recv.at[zs, h])
                send(x_half(zs, there, h), x_half(zs, there, h), xp_send, xp_recv.at[zs, 1, h], z, pal)
    @pl.loop(0, ND)
    def _(j):
        for r in range(2):
            t = jnp.where(r < counts[0, 0, j], ids[0, 0, 2 * j + r], -1)
            tag[j, r : r + 1, :] = jnp.full((1, tag.shape[2]), t, jnp.int32)

    got_tag[d] = tag[d]
    acc[...] = jnp.zeros_like(acc)
    w_load.wait()

    def weight_step(i, total):
        v = w[0, pl.ds(pl.multiple_of(i * 8, 8), 8), :]
        v = v * v
        for k in range(cols // 128):
            total = total + v[:, k * 128 : (k + 1) * 128]
        return total

    weight_sq = lax.fori_loop(0, rows // 8, weight_step, jnp.zeros((8, 128), jnp.float32))
    @pl.when(core == 0)
    def _():
        @pl.loop(0, NZ + 6)
        def _(it):
            @pl.when(it < NZ)
            def _():
                zs = column(it)
                landed(it)
                push(whole(zs, duo, 0), zs, 0, right)
                push(whole(zs, duo, 0), zs, 1, left)
                push(whole(zs, duo, 0), zs, 4, inner)

            @pl.when(it == 1)
            def _():
                relay()

            @pl.when((it >= 1) & (it < NZ + 1))
            def _():
                zs = column(it - 1)
                arrived(whole(zs, duo, -1), ag_recv.at[zs, 0])
                push(part(zs, duo, -1, 0), zs, 2, right)
                push(whole(zs, duo, -1), zs, 5, inner)
                arrived(whole(zs, duo, 1), ag_recv.at[zs, 1])
                push(part(zs, duo, 1, 1), zs, 3, left)
                push(whole(zs, duo, 1), zs, 6, inner)

            @pl.when((it >= 2) & (it < NZ + 2))
            def _():
                zs = column(it - 2)
                for h in range(2):
                    arrived(part(zs, duo, 2, h), ag_recv.at[zs, 2 + h])
                push(whole(zs, duo, 2), zs, 7, inner)

            @pl.when((it >= 3) & (it < NZ + 3))
            def _():
                zs = column(it - 3)
                for k, da in enumerate((0, -1, 1, 2)):
                    arrived(whole(zs, 1 - duo, da), ag_recv.at[zs, 4 + k])

            x_stages(it)

    @pl.when(core == 1)
    def _():
        @pl.loop(0, NZ + 6)
        def _(it):
            @pl.when(it < NZ)
            def _():
                zs = column(it)
                landed(it)
                push(whole(zs, duo, 0), zs, 4, inner)
                push(whole(zs, duo, 0), zs, 0, right)
                push(whole(zs, duo, 0), zs, 1, left)

            @pl.when(it == 1)
            def _():
                relay()

            @pl.when((it >= 1) & (it < NZ + 1))
            def _():
                zs = column(it - 1)
                arrived(whole(zs, 1 - duo, 0), ag_recv.at[zs, 4])
                push(whole(zs, 1 - duo, 0), zs, 5, right)
                push(whole(zs, 1 - duo, 0), zs, 6, left)
                arrived(whole(zs, duo, -1), ag_recv.at[zs, 0])
                push(part(zs, duo, -1, 0), zs, 2, right)
                arrived(whole(zs, duo, 1), ag_recv.at[zs, 1])
                push(part(zs, duo, 1, 1), zs, 3, left)

            @pl.when((it >= 2) & (it < NZ + 2))
            def _():
                zs = column(it - 2)
                arrived(whole(zs, 1 - duo, -1), ag_recv.at[zs, 5])
                push(part(zs, 1 - duo, -1, 0), zs, 7, right)
                arrived(whole(zs, 1 - duo, 1), ag_recv.at[zs, 6])
                push(part(zs, 1 - duo, 1, 1), zs, 8, left)
                for h in range(2):
                    arrived(part(zs, duo, 2, h), ag_recv.at[zs, 2 + h])

            @pl.when((it >= 3) & (it < NZ + 3))
            def _():
                zs = column(it - 3)
                for h in range(2):
                    arrived(part(zs, 1 - duo, 2, h), ag_recv.at[zs, 7 + h])

            x_stages(it)
    def grad_step(i, total):
        v = acc[pl.ds(pl.multiple_of(i * 8, 8), 8), :]
        v = v * v
        for k in range(quarter // 128):
            total = total + v[:, k * 128 : (k + 1) * 128]
        return total

    grad_sq = lax.fori_loop(0, 4 * rows // 8, grad_step, jnp.zeros((8, 128), jnp.float32))
    norms[d, 0:1] = jnp.sum(weight_sq, axis=0, keepdims=True)
    norms[d, 1:2] = jnp.sum(grad_sq, axis=0, keepdims=True)

    grad[:, pl.ds(pl.multiple_of(me * quarter, quarter), quarter)] = acc[pl.ds(me * rows, rows), :]

    @pl.loop(1, ND)
    def _(p):
        send(norms.at[d], norms.at[d], norm_send, norm_recv.at[d], z, (d + p) % ND)
    mates = (
        (me, d),
        (side * 2 + 1 - core, pal),
        ((1 - side) * 2 + core, outer),
        ((1 - side) * 2 + 1 - core, outer + 1 - 2 * core),
    )

    def columns(k):
        return pl.ds(pl.multiple_of(mates[k][0] * quarter, quarter), quarter)

    for k in range(1, 4):
        send(
            acc.at[pl.ds(mates[k][0] * rows, rows)],
            grad.at[:, columns(0)],
            half_send,
            half_recv.at[k - 1],
            z,
            mates[k][1],
        )

    def block_out(j):
        send(tag.at[j], got_tag.at[d], tag_send, tag_recv.at[d], z, j)
        send(
            bg_hbm.at[0, 0, pl.ds(2 * j, 2)],
            got.at[pl.ds(2 * d, 2)],
            bg_send,
            bg_recv.at[d],
            z,
            j,
        )

    near = ND // 2

    @pl.loop(1, near)
    def _(p):
        block_out(side * near + (d + p) % near)
    m_load.wait()

    @pl.loop(1, ND)
    def _(p):
        j = (d + p) % ND
        arrived(norms.at[j], norm_recv.at[j])
    totals = jnp.sum(norms[...], axis=0)
    weight_total = jnp.sum(totals[0:1], keepdims=True)
    grad_total = jnp.sum(totals[1:2], keepdims=True)
    weight_norm = jnp.sqrt(weight_total + eps_norm)
    trust = weight_norm / (jnp.sqrt(grad_total + eps_norm) + tower_decay * weight_norm)
    scale = tower_rate * trust

    strip = 16
    up = (z + 1) % NZ
    down = (z + NZ - 1) % NZ

    def piece(s, k):
        return slabs.at[s, :, columns(k)]

    def renew(k):
        @pl.loop(0, rows // strip)
        def _(i):
            at = pl.ds(pl.multiple_of(i * strip, strip), strip)
            old = w[0, at, columns(k)]
            new_m = momentum_keep * m[0, at, columns(k)] + scale * (
                grad[at, columns(k)] + tower_decay * old
            )
            new_w = old - new_m
            m[0, at, columns(k)] = new_m
            w[0, at, columns(k)] = new_w
            slabs[z, at, columns(k)] = new_w.astype(jnp.bfloat16)

        send(piece(z, k), piece(z, k), wz_send, wz_recv.at[0, 0, k], up, d)
        send(piece(z, k), piece(z, k), wz_send, wz_recv.at[1, 0, k], down, d)

    def onward(j, ks):
        low = (z + NZ - j) % NZ
        high = (z + j) % NZ
        for k in ks:
            if j < 3 or k % 2 == 0:
                arrived(piece(low, k), wz_recv.at[0, j - 1, k])
                send(piece(low, k), piece(low, k), wz_send, wz_recv.at[0, j, k], up, d)
            if j < 3 or k % 2 == 1:
                arrived(piece(high, k), wz_recv.at[1, j - 1, k])
                send(piece(high, k), piece(high, k), wz_send, wz_recv.at[1, j, k], down, d)
    renew(0)
    arrived(grad.at[:, columns(1)], half_recv.at[0])
    renew(1)
    onward(1, (0, 1))
    arrived(grad.at[:, columns(2)], half_recv.at[1])
    renew(2)
    onward(2, (0, 1))
    arrived(grad.at[:, columns(3)], half_recv.at[2])
    renew(3)
    @pl.loop(0, near)
    def _(p):
        block_out((1 - side) * near + (d + p) % near)
    onward(1, (2, 3))
    onward(3, (0, 1))
    onward(2, (2, 3))
    onward(3, (2, 3))
    own_load.wait()
    t_load.wait()

    @pl.loop(1, ND)
    def _(p):
        j = (d + p) % ND
        arrived(got.at[pl.ds(2 * j, 2)], bg_recv.at[j])
        arrived(got_tag.at[j], tag_recv.at[j])
    nb = table.shape[1]
    wide = table.shape[3]
    lane = lax.broadcasted_iota(jnp.int32, (strip, wide), 1)
    same = lane % strip == lax.broadcasted_iota(jnp.int32, (strip, wide), 0)
    names = lane // strip

    @pl.loop(0, ND)
    def _(s):
        for r in range(2):
            hit = (got_tag[s, r : r + 1, :] == names) & same
            pick[2 * s + r] = jnp.where(hit, 1.0, 0.0).astype(jnp.bfloat16)

    turned[...] = pick[...].reshape(2 * ND * strip, wide).T

    @pl.loop(0, table.shape[2] // strip)
    def _(i):
        at = pl.ds(pl.multiple_of(i * strip, strip), strip)
        values = got[:, at, :].reshape(2 * ND * strip, wide)
        total = jnp.dot(turned[...], values, preferred_element_type=jnp.float32)
        sums[:, at, :] = total.reshape(nb, strip, wide)

    tags = got_tag[:, 0:2, :]
    for b in range(nb):
        hits = jnp.sum(jnp.where(tags == b, 1.0, 0.0), axis=(0, 1)).reshape(1, wide)
        flat = table[0, b]
        total = sums[b]
        w_norm = jnp.sqrt(jnp.sum(flat * flat, keepdims=True) + eps_norm)
        g_norm = jnp.sqrt(jnp.sum(total * total, keepdims=True) + eps_norm)
        block_trust = w_norm / (g_norm + table_decay * w_norm)
        moved = flat - table_rate * block_trust * (total + table_decay * flat)
        table[0, b] = jnp.where(hits > 0, moved, flat)
    low = (z + NZ - 3) % NZ
    high = (z + 3) % NZ
    for k in range(4):
        if k % 2 == 0:
            arrived(piece(high, k), wz_recv.at[1, 2, k])
            arrived(piece(far, k), wz_recv.at[0, 3, k])
        else:
            arrived(piece(low, k), wz_recv.at[0, 2, k])
            arrived(piece(far, k), wz_recv.at[1, 3, k])
    arrived(g_slot.at[0:6], gz_send)
    for k in range(3):
        arrived(g_slot.at[0, 0], go_send.at[k])
    arrived(g_relay, gr_send)
    arrived(g_relay, gf_send)
    arrived(x_slot.at[0:6], xz_send)
    arrived(x_relay, xr_send)
    arrived(x_relay, xf_send)
    arrived(x_all.at[:, 0], xo_send)
    arrived(x_all.at[:, 0:2], xp_send)
    arrived(g_all.at[0:7], ag_send)
    arrived(acc.at[0 : 3 * rows], half_send)
    arrived(norms.at[0 : ND - 1], norm_send)
    arrived(got.at[0 : 2 * (ND - 1)], bg_send)
    arrived(tag.at[0 : ND - 1], tag_send)
    arrived(slabs.at[0:7], wz_send)


def finish_kernel(owner, slots, new_w, new_m, new_t, out, w_out, m_out, t_out, sem):
    copies = [
        pltpu.make_async_copy(slots.at[owner[l]], out.at[l], sem.at[l])
        for l in range(out.shape[0])
    ] + [
        pltpu.make_async_copy(new_w, w_out, sem.at[NZ]),
        pltpu.make_async_copy(new_m, m_out, sem.at[NZ + 1]),
        pltpu.make_async_copy(new_t, t_out, sem.at[NZ + 2]),
    ]
    for copy in copies:
        copy.start()
    for copy in copies:
        copy.wait()


def local(
    layer_inputs,
    output_grads,
    layer_owner,
    master_weights,
    momentum,
    table_blocks,
    block_grads,
    block_ids,
    block_counts,
):
    layers, tokens, rows = layer_inputs.shape
    per, cols = output_grads.shape[1:]
    quarter = cols // 4
    nb, tall, wide = table_blocks.shape[1:]
    f32, bf16, i32 = jnp.float32, jnp.bfloat16, jnp.int32
    hbm = pl.BlockSpec(memory_space=pltpu.HBM)
    smem = pl.BlockSpec(memory_space=pltpu.SMEM)
    anywhere = pl.BlockSpec(memory_space=pl.ANY)
    dma = pltpu.SemaphoreType.DMA
    slots, new_w, new_m, new_t = pl.pallas_call(
        step_kernel,
        name="step",
        out_shape=(
            pltpu.VMEM((NZ, rows, cols), bf16),
            pltpu.VMEM(master_weights.shape, f32),
            pltpu.VMEM(momentum.shape, f32),
            pltpu.VMEM(table_blocks.shape, f32),
        ),
        in_specs=[smem, smem, smem] + [hbm] * 6,
        out_specs=(pl.BlockSpec(memory_space=pltpu.VMEM),) * 4,
        scratch_shapes=[
            pltpu.VMEM((layers, tokens, rows), bf16),
            pltpu.VMEM((layers, tokens, rows), bf16),
            pltpu.VMEM((NZ, 4, tokens, rows), bf16),
            pltpu.VMEM((4 * rows, tokens), bf16),
            pltpu.VMEM((2, tokens // 2, rows), bf16),
            pltpu.VMEM((layers, per, cols), bf16),
            pltpu.VMEM((layers, 4, per, quarter), bf16),
            pltpu.VMEM((NZ, 2, 2, NX, 2 * per, quarter), bf16),
            pltpu.VMEM((2, 2, per, quarter), bf16),
            pltpu.VMEM((4 * rows, quarter), f32),
            pltpu.VMEM((rows, cols), f32),
            pltpu.VMEM((nb, tall, wide), f32),
            pltpu.VMEM((2 * ND, wide // nb, wide), bf16),
            pltpu.VMEM((wide, 2 * ND * (wide // nb)), bf16),
            pltpu.VMEM((2 * ND, tall, wide), bf16),
            pltpu.VMEM((ND, 8, wide), i32),
            pltpu.VMEM((ND, 8, wide), i32),
            pltpu.VMEM((ND, 2, 128), f32),
            dma((6,)),
            dma,
            dma((NZ, 4)),
            dma((3,)),
            dma,
            dma((2,)),
            dma,
            dma,
            dma((NZ, 2)),
            dma,
            dma((2,)),
            dma,
            dma,
            dma((NZ, 2)),
            dma,
            dma((NZ, 2, 2)),
            dma,
            dma((NZ, 9)),
            dma,
            dma((3,)),
            dma,
            dma((ND,)),
            dma,
            dma((ND,)),
            dma,
            dma((ND,)),
            dma,
            dma((2, 4, 4)),
        ],
        compiler_params=pltpu.CompilerParams(
            collective_id=0, has_side_effects=True, vmem_limit_bytes=60_160_000
        ),
    )(
        layer_owner,
        block_ids,
        block_counts,
        layer_inputs,
        output_grads,
        master_weights,
        momentum,
        table_blocks,
        block_grads,
    )
    new_weights, new_master, new_moment, new_table = pl.pallas_call(
        finish_kernel,
        name="finish",
        in_specs=[smem] + [anywhere] * 4,
        out_specs=(hbm,) * 4,
        scratch_shapes=[dma((layers + 3,))],
        out_shape=(
            jax.ShapeDtypeStruct((layers, rows, cols), bf16),
            jax.ShapeDtypeStruct(master_weights.shape, f32),
            jax.ShapeDtypeStruct(momentum.shape, f32),
            jax.ShapeDtypeStruct(table_blocks.shape, f32),
        ),
        compiler_params=pltpu.CompilerParams(vmem_limit_bytes=1024 * 1024),
    )(layer_owner, slots, new_w, new_m, new_t)
    return new_master, new_moment, new_weights, new_table


def solution(mesh):
    return jax.shard_map(
        local,
        mesh=mesh,
        in_specs=(
            P(None, "grp", "dev"),
            P(None, ("grp", "dev"), None),
            P(),
            P("grp", "dev", None),
            P("grp", "dev", None),
            P("grp", "dev", None, None),
            P("grp", "dev", None, None, None),
            P("grp", "dev", None),
            P("grp", "dev", None),
        ),
        out_specs=(
            P("grp", "dev", None),
            P("grp", "dev", None),
            P(None, "dev", None),
            P("grp", "dev", None, None),
        ),
        check_vma=False,
    )
```

```python
import functools

import jax
import jax.numpy as jnp
from jax import lax
from jax.experimental import pallas as pl
from jax.experimental.pallas import tpu as pltpu
from jax.sharding import PartitionSpec as P

tower_rate = 0.5
momentum_keep = 0.9
tower_decay = 0.1
table_rate = 0.5
table_decay = 0.2
eps_norm = 1e-06

NZ = 8
NX = 4
NY = 4
ND = NX * NY * 2


def step_kernel(
    owner,
    ids,
    counts,
    x_hbm,
    g_hbm,
    w_hbm,
    m_hbm,
    t_hbm,
    bg_hbm,
    slabs,
    w,
    m,
    table,
    x_in,
    x_slot,
    x_all,
    x_turn,
    x_relay,
    g_in,
    g_slot,
    g_other,
    g_all,
    g_relay,
    acc,
    grad,
    sums,
    pick,
    turned,
    got,
    tag,
    got_tag,
    norms,
    in_sem,
    gz_send,
    gz_recv,
    go_send,
    gx_send,
    gx_recv,
    gr_send,
    gr_recv,
    gf_send,
    xz_send,
    xz_recv,
    xr_send,
    xr_recv,
    xf_send,
    xo_send,
    xo_recv,
    xp_send,
    xp_recv,
    ag_send,
    ag_recv,
    half_send,
    half_recv,
    norm_send,
    norm_recv,
    bg_send,
    bg_recv,
    tag_send,
    tag_recv,
    wz_send,
    wz_recv,
):
    z = lax.axis_index("grp")
    d = lax.axis_index("dev")
    core = d % 2
    cx = (d // 2) % NX
    cy = d // (2 * NX)
    chip = d // 2
    side = cy // 2
    duo = ((cy + 1) // 2) % 2
    oy = NY - 1 - cy
    iy = cy + 1 - 2 * (cy % 2)
    me = side * 2 + core
    pal = chip * 2 + 1 - core
    outer = (oy * NX + cx) * 2 + core
    inner = (iy * NX + cx) * 2 + core
    right = (cy * NX + (cx + 1) % NX) * 2 + core
    left = (cy * NX + (cx + NX - 1) % NX) * 2 + core
    rows = w_hbm.shape[1]
    cols = w_hbm.shape[2]
    quarter = cols // 4
    per = g_hbm.shape[1]
    tokens = x_hbm.shape[1]
    band = tokens // NY

    def send(src, dst, s_sem, r_sem, zz, dd):
        pltpu.make_async_remote_copy(
            src_ref=src,
            dst_ref=dst,
            send_sem=s_sem,
            recv_sem=r_sem,
            device_id=(zz, dd),
            device_id_type=pl.DeviceIdType.MESH,
        ).start()

    def arrived(ref, sem):
        pltpu.make_async_copy(ref, ref, sem).wait()

    def column(i):
        off = (i % 2) * ((i + 1) // 2) + (1 - i % 2) * (NZ - i // 2)
        return (z + off) % NZ

    g_load = pltpu.make_async_copy(g_hbm, g_in, in_sem.at[1])
    x_load = pltpu.make_async_copy(x_hbm, x_in, in_sem.at[0])
    w_load = pltpu.make_async_copy(w_hbm.at[0], w.at[0], in_sem.at[2])
    m_load = pltpu.make_async_copy(m_hbm.at[0], m.at[0], in_sem.at[3])
    t_load = pltpu.make_async_copy(t_hbm.at[0], table.at[0], in_sem.at[4])
    own_load = pltpu.make_async_copy(
        bg_hbm.at[0, 0, pl.ds(2 * d, 2)], got.at[pl.ds(2 * d, 2)], in_sem.at[5]
    )
    g_load.start()
    barrier = pltpu.get_barrier_semaphore()

    @pl.loop(1, ND)
    def _(p):
        pl.semaphore_signal(
            barrier, inc=1, device_id=(z, (d + p) % ND), device_id_type=pl.DeviceIdType.MESH
        )

    @pl.loop(1, NZ)
    def _(p):
        for cc in range(2):
            pl.semaphore_signal(
                barrier,
                inc=1,
                device_id=((z + p) % NZ, chip * 2 + cc),
                device_id_type=pl.DeviceIdType.MESH,
            )

    x_load.start()
    w_load.start()
    m_load.start()
    t_load.start()
    own_load.start()

    def layer_of(s):
        found = jnp.int32(0)
        for l in range(NZ):
            found = jnp.where(owner[l] == s, l, found)
        return found
    g_load.wait()

    @pl.loop(0, NZ)
    def _(s):
        l = layer_of(s)
        for q in range(4):
            g_slot[s, q] = g_in[l, :, q * quarter : (q + 1) * quarter]

    g_all[z, duo, side, cx, pl.ds(core * per, per), :] = g_slot[z, me]
    pl.semaphore_wait(barrier, ND - 1 + 2 * (NZ - 1))
    def g_home(zs):
        return g_all.at[zs, duo, side, cx, pl.ds(core * per, per)]

    far = (z + NZ // 2) % NZ
    ways = (1, NZ - 1)
    deep = tokens // 2
    there = (1 - side) * 2 + core
    mine = pl.ds(2 * side, 2)
    theirs = pl.ds(2 * (1 - side), 2)

    def g_there(zs):
        return g_all.at[zs, duo, 1 - side, cx, pl.ds(core * per, per)]

    send(g_slot.at[z, side * 2 + 1 - core], g_home(z), go_send.at[0], gz_recv.at[z], z, pal)
    for cc in range(2):
        send(
            g_slot.at[z, (1 - side) * 2 + cc],
            g_home(z),
            go_send.at[1 + cc],
            gz_recv.at[z],
            z,
            (oy * NX + cx) * 2 + cc,
        )

    def g_cross(zt):
        send(g_slot.at[zt, theirs], g_other.at[zt], gx_send, gx_recv.at[zt], z, outer)

    g_cross((z + 1) % NZ)
    g_cross((z + NZ - 1) % NZ)
    g_cross(far)
    for j in (2, 3):
        g_cross((z + j) % NZ)
        g_cross((z + NZ - j) % NZ)

    send(g_slot.at[far, mine], g_relay.at[0], gr_send, gr_recv.at[0], (z + 1) % NZ, d)
    def g_own(j):
        for zt in ((z + j) % NZ, (z + NZ - j) % NZ):
            for cc in range(2):
                send(
                    g_slot.at[zt, 2 * side + cc],
                    g_home(z),
                    gz_send,
                    gz_recv.at[z],
                    zt,
                    chip * 2 + cc,
                )

    def g_for_other(j):
        for zt in ((z + j) % NZ, (z + NZ - j) % NZ):
            arrived(g_other.at[zt], gx_recv.at[zt])
            for cc in range(2):
                send(
                    g_other.at[zt, cc], g_there(z), gz_send, gz_recv.at[z], zt, chip * 2 + cc
                )

    def x_out(j):
        for h in range(2):
            for zt in ((z + j) % NZ, (z + NZ - j) % NZ):
                at = pl.ds(h * deep, deep)
                send(
                    x_slot.at[zt, at], x_all.at[z, me, at], xz_send, xz_recv.at[z, h], zt, d
                )

    def x_half(zs, s, h):
        return x_all.at[zs, s, pl.ds(pl.multiple_of(h * deep, deep), deep)]

    def x_share(zs, h):
        ref = x_half(zs, me, h)
        send(ref, ref, xo_send, xo_recv.at[zs, h], z, outer)
        send(ref, ref, xp_send, xp_recv.at[zs, h], z, pal)

    def x_first(j, h):
        for zs in ((z + j) % NZ, (z + NZ - j) % NZ):
            arrived(x_half(zs, me, h), xz_recv.at[zs, h])
            x_share(zs, h)

    def x_first_far(h):
        arrived(x_half(far, me, h), xz_recv.at[far, h])
        x_share(far, h)

    def x_second(zs, h):
        ref = x_half(zs, there, h)
        arrived(ref, xo_recv.at[zs, h])
        send(ref, ref, xp_send, xp_recv.at[zs, h], z, pal)

    def x_second_both(j, h):
        for zs in ((z + j) % NZ, (z + NZ - j) % NZ):
            x_second(zs, h)

    g_own(1)
    g_own(2)

    x_load.wait()

    @pl.loop(0, NZ)
    def _(s):
        l = layer_of(s)
        x_slot[s] = x_in[l]

    x_all[z, me] = x_slot[z]

    for way in range(2):
        for h in range(2):
            send(
                x_slot.at[far, pl.ds((2 * h + way) * band, band)],
                x_relay.at[way, h],
                xr_send,
                xr_recv.at[way, h],
                (z + ways[way]) % NZ,
                d,
            )

    for h in range(2):
        x_share(z, h)

    def whole(zs, pr, da):
        return g_all.at[zs, pr, :, (cx + da + NX) % NX]

    def part(zs, pr, da, h):
        return g_all.at[zs, pr, h, (cx + da + NX) % NX]

    def push(ref, zs, k, dd):
        send(ref, ref, ag_send, ag_recv.at[zs, k], z, dd)

    def landed(it):
        zs = column(it)

        @pl.when(it == 0)
        def _():
            arrived(g_slot.at[0, 0:3], gz_recv.at[zs])

        @pl.when(it > 0)
        def _():
            arrived(g_slot.at[0], gz_recv.at[zs])

    def feed(it):
        @pl.when(it == 0)
        def _():
            g_for_other(1)
            x_out(1)
            arrived(g_other.at[far], gx_recv.at[far])
            send(g_other.at[far], g_relay.at[1], gr_send, gr_recv.at[1], (z + NZ - 1) % NZ, d)

        @pl.when(it == 1)
        def _():
            g_for_other(2)
            g_own(3)
            g_for_other(3)
            x_out(2)

        @pl.when(it == 2)
        def _():
            relay()

    def relay():
        for way in range(2):
            zs = (z + NZ - ways[way]) % NZ
            zt = (zs + NZ // 2) % NZ
            arrived(g_relay.at[way], gr_recv.at[way])
            home = g_home(zs) if way == 0 else g_there(zs)
            sem = gz_recv.at[zs]
            for cc in range(2):
                send(g_relay.at[way, cc], home, gf_send, sem, zt, chip * 2 + cc)

        x_out(3)
        for way in range(2):
            zs = (z + NZ - ways[way]) % NZ
            zt = (zs + NZ // 2) % NZ
            for h in range(2):
                arrived(x_relay.at[way, h], xr_recv.at[way, h])
                send(
                    x_relay.at[way, h],
                    x_all.at[zs, me, pl.ds((2 * h + way) * band, band)],
                    xf_send,
                    xz_recv.at[zs, h],
                    zt,
                    d,
                )

    def multiply(u):
        k = u // 2
        h = u % 2
        zs = column(k)
        arrived(x_slot.at[0], xp_recv.at[zs, h])
        @pl.loop(0, 4)
        def _(s):
            for pr in range(2):
                y = pr + h * (NY - 1 - 2 * pr)
                x_turn[pl.ds(s * rows, rows), pr * band : (pr + 1) * band] = x_all[
                    zs, s, pl.ds(pl.multiple_of(y * band, band), band), :
                ].T

        @pl.loop(0, quarter // 256)
        def _(n):
            where = pl.ds(pl.multiple_of(n * 256, 256), 256)
            block = g_all[zs, :, h, :, :, where].reshape(deep, 256)
            acc[:, where] += jnp.dot(x_turn[...], block, preferred_element_type=jnp.float32)

    def x_stages(it):
        @pl.when(it == 2)
        def _():
            for h in range(2):
                x_second(z, h)

        def event(steps, do):
            for when, *what in steps:

                @pl.when(it == when)
                def _():
                    do(*what)

        event(
            ((3, 1, 0), (4, 1, 1), (5, 2, 0), (6, 2, 1), (8, 3, 0), (9, 3, 1)),
            x_first,
        )
        event(
            ((5, 1, 0), (6, 1, 1), (7, 2, 0), (8, 2, 1), (10, 3, 0), (11, 3, 1)),
            x_second_both,
        )
        event(((10, 0), (10, 1)), x_first_far)
        event(((12, far, 0), (13, far, 1)), x_second)

        first = jnp.where(
            it < 7, 0, jnp.where(it < 12, 2 * it - 12, it + 1)
        )
        count = jnp.where(
            it == 11, 3, jnp.where(it == 12, 1, jnp.where((it == 4) | (it >= 7), 2, 0))
        )

        @pl.loop(first, first + count)
        def _(v):
            multiply(v + jnp.where(v == 11, 1, 0) - jnp.where(v == 12, 1, 0))
    @pl.loop(0, ND)
    def _(j):
        for r in range(2):
            t = jnp.where(r < counts[0, 0, j], ids[0, 0, 2 * j + r], -1)
            tag[j, r : r + 1, :] = jnp.full((1, tag.shape[2]), t, jnp.int32)

    got_tag[d] = tag[d]
    acc[...] = jnp.zeros_like(acc)
    w_load.wait()

    def weight_step(i, total):
        v = w[0, pl.ds(pl.multiple_of(i * 8, 8), 8), :]
        v = v * v
        for k in range(cols // 128):
            total = total + v[:, k * 128 : (k + 1) * 128]
        return total

    weight_sq = lax.fori_loop(0, rows // 8, weight_step, jnp.zeros((8, 128), jnp.float32))
    @pl.when(core == 0)
    def _():
        @pl.loop(0, NZ + 6)
        def _(it):
            @pl.when(it < NZ)
            def _():
                zs = column(it)
                landed(it)
                push(whole(zs, duo, 0), zs, 0, right)
                push(whole(zs, duo, 0), zs, 1, left)
                push(whole(zs, duo, 0), zs, 3, inner)

            @pl.when((it >= 1) & (it < NZ + 1))
            def _():
                zs = column(it - 1)
                arrived(whole(zs, duo, -1), ag_recv.at[zs, 0])
                push(part(zs, duo, -1, 0), zs, 2, right)
                push(whole(zs, duo, -1), zs, 3, inner)
                arrived(whole(zs, duo, 1), ag_recv.at[zs, 1])
                push(part(zs, duo, 1, 1), zs, 2, left)
                push(whole(zs, duo, 1), zs, 3, inner)

            feed(it)

            @pl.when((it >= 2) & (it < NZ + 2))
            def _():
                zs = column(it - 2)
                arrived(whole(zs, duo, 2), ag_recv.at[zs, 2])
                push(whole(zs, duo, 2), zs, 3, inner)

            @pl.when((it >= 3) & (it < NZ + 3))
            def _():
                zs = column(it - 3)
                arrived(g_all.at[zs, 1 - duo], ag_recv.at[zs, 3])

            x_stages(it)

    @pl.when(core == 1)
    def _():
        @pl.loop(0, NZ + 6)
        def _(it):
            @pl.when(it < NZ)
            def _():
                zs = column(it)
                landed(it)
                push(whole(zs, duo, 0), zs, 3, inner)
                push(whole(zs, duo, 0), zs, 0, right)
                push(whole(zs, duo, 0), zs, 1, left)

            @pl.when((it >= 1) & (it < NZ + 1))
            def _():
                zs = column(it - 1)
                arrived(whole(zs, 1 - duo, 0), ag_recv.at[zs, 3])
                push(whole(zs, 1 - duo, 0), zs, 4, right)
                push(whole(zs, 1 - duo, 0), zs, 5, left)
                arrived(whole(zs, duo, -1), ag_recv.at[zs, 0])
                push(part(zs, duo, -1, 0), zs, 2, right)
                arrived(whole(zs, duo, 1), ag_recv.at[zs, 1])
                push(part(zs, duo, 1, 1), zs, 2, left)

            feed(it)

            @pl.when((it >= 2) & (it < NZ + 2))
            def _():
                zs = column(it - 2)
                arrived(whole(zs, 1 - duo, -1), ag_recv.at[zs, 4])
                push(part(zs, 1 - duo, -1, 0), zs, 6, right)
                arrived(whole(zs, 1 - duo, 1), ag_recv.at[zs, 5])
                push(part(zs, 1 - duo, 1, 1), zs, 6, left)
                arrived(whole(zs, duo, 2), ag_recv.at[zs, 2])

            @pl.when((it >= 3) & (it < NZ + 3))
            def _():
                zs = column(it - 3)
                arrived(whole(zs, 1 - duo, 2), ag_recv.at[zs, 6])

            x_stages(it)
    def grad_step(i, total):
        for k in range(4):
            v = acc[pl.ds(pl.multiple_of(i * 32 + k * 8, 8), 8), :]
            total = total + v * v
        return total

    wide_sq = lax.fori_loop(0, 4 * rows // 32, grad_step, jnp.zeros((8, quarter), jnp.float32))
    grad_sq = wide_sq[:, 0:128]
    for k in range(1, quarter // 128):
        grad_sq = grad_sq + wide_sq[:, k * 128 : (k + 1) * 128]
    norms[d, 0:1] = jnp.sum(weight_sq, axis=0, keepdims=True)
    norms[d, 1:2] = jnp.sum(grad_sq, axis=0, keepdims=True)
    grad[:, pl.ds(pl.multiple_of(me * quarter, quarter), quarter)] = acc[pl.ds(me * rows, rows), :]

    @pl.loop(1, ND)
    def _(p):
        send(norms.at[d], norms.at[d], norm_send, norm_recv, z, (d + p) % ND)
    mates = (
        (me, d),
        (side * 2 + 1 - core, pal),
        ((1 - side) * 2 + core, outer),
        ((1 - side) * 2 + 1 - core, outer + 1 - 2 * core),
    )

    def columns(k):
        return pl.ds(pl.multiple_of(mates[k][0] * quarter, quarter), quarter)

    for k in range(1, 4):
        send(
            acc.at[pl.ds(mates[k][0] * rows, rows)],
            grad.at[:, columns(0)],
            half_send,
            half_recv.at[k - 1],
            z,
            mates[k][1],
        )

    def block_out(j):
        send(tag.at[j], got_tag.at[d], tag_send, tag_recv, z, j)
        send(
            bg_hbm.at[0, 0, pl.ds(2 * j, 2)],
            got.at[pl.ds(2 * d, 2)],
            bg_send,
            bg_recv,
            z,
            j,
        )

    near = ND // 2
    m_load.wait()

    arrived(norms.at[0 : ND - 1], norm_recv)
    totals = jnp.sum(norms[...], axis=0)
    weight_total = jnp.sum(totals[0:1], keepdims=True)
    grad_total = jnp.sum(totals[1:2], keepdims=True)
    weight_norm = jnp.sqrt(weight_total + eps_norm)
    trust = weight_norm / (jnp.sqrt(grad_total + eps_norm) + tower_decay * weight_norm)
    scale = tower_rate * trust

    strip = 16
    up = (z + 1) % NZ
    down = (z + NZ - 1) % NZ

    def piece(s, k):
        return slabs.at[s, mates[k][0]]

    def renew(k):
        @pl.loop(0, rows // strip)
        def _(i):
            at = pl.ds(pl.multiple_of(i * strip, strip), strip)
            old = w[0, at, columns(k)]
            new_m = momentum_keep * m[0, at, columns(k)] + scale * (
                grad[at, columns(k)] + tower_decay * old
            )
            new_w = old - new_m
            m[0, at, columns(k)] = new_m
            w[0, at, columns(k)] = new_w
            slabs[z, mates[k][0], at, :] = new_w.astype(jnp.bfloat16)

        send(piece(z, k), piece(z, k), wz_send, wz_recv.at[0, 0, k], up, d)
        send(piece(z, k), piece(z, k), wz_send, wz_recv.at[1, 0, k], down, d)

    def onward(j, ks):
        low = (z + NZ - j) % NZ
        high = (z + j) % NZ
        for k in ks:
            if j < 3 or k % 2 == 0:
                arrived(piece(low, k), wz_recv.at[0, j - 1, k])
                send(piece(low, k), piece(low, k), wz_send, wz_recv.at[0, j, k], up, d)
            if j < 3 or k % 2 == 1:
                arrived(piece(high, k), wz_recv.at[1, j - 1, k])
                send(piece(high, k), piece(high, k), wz_send, wz_recv.at[1, j, k], down, d)
    renew(0)
    arrived(grad.at[:, columns(1)], half_recv.at[0])
    renew(1)

    @pl.loop(1, near)
    def _(p):
        block_out(side * near + (d + p) % near)
    onward(1, (0,))
    arrived(grad.at[:, columns(2)], half_recv.at[1])
    renew(2)
    onward(1, (1,))
    onward(2, (0,))
    arrived(grad.at[:, columns(3)], half_recv.at[2])
    renew(3)
    @pl.loop(0, near)
    def _(p):
        block_out((1 - side) * near + (d + p) % near)
    onward(2, (1,))
    onward(1, (2, 3))
    onward(3, (0, 1))
    onward(2, (2, 3))
    onward(3, (2, 3))
    own_load.wait()
    t_load.wait()

    arrived(got.at[0 : 2 * (ND - 1)], bg_recv)
    arrived(got_tag.at[0 : ND - 1], tag_recv)
    nb = table.shape[1]
    wide = table.shape[3]
    lane = lax.broadcasted_iota(jnp.int32, (strip, wide), 1)
    same = lane % strip == lax.broadcasted_iota(jnp.int32, (strip, wide), 0)
    names = lane // strip

    @pl.loop(0, ND)
    def _(s):
        for r in range(2):
            hit = (got_tag[s, r : r + 1, :] == names) & same
            pick[2 * s + r] = jnp.where(hit, 1.0, 0.0).astype(jnp.bfloat16)

    turned[...] = pick[...].reshape(2 * ND * strip, wide).T

    @pl.loop(0, table.shape[2] // strip)
    def _(i):
        at = pl.ds(pl.multiple_of(i * strip, strip), strip)
        values = got[:, at, :].reshape(2 * ND * strip, wide)
        total = jnp.dot(turned[...], values, preferred_element_type=jnp.float32)
        sums[:, at, :] = total.reshape(nb, strip, wide)

    tags = got_tag[:, 0:2, :]
    for b in range(nb):
        hits = jnp.sum(jnp.where(tags == b, 1.0, 0.0), axis=(0, 1)).reshape(1, wide)
        flat = table[0, b]
        total = sums[b]
        w_norm = jnp.sqrt(jnp.sum(flat * flat, keepdims=True) + eps_norm)
        g_norm = jnp.sqrt(jnp.sum(total * total, keepdims=True) + eps_norm)
        block_trust = w_norm / (g_norm + table_decay * w_norm)
        moved = flat - table_rate * block_trust * (total + table_decay * flat)
        table[0, b] = jnp.where(hits > 0, moved, flat)
    low = (z + NZ - 3) % NZ
    high = (z + 3) % NZ
    for k in range(4):
        if k % 2 == 0:
            arrived(piece(high, k), wz_recv.at[1, 2, k])
            arrived(piece(far, k), wz_recv.at[0, 3, k])
        else:
            arrived(piece(low, k), wz_recv.at[0, 2, k])
            arrived(piece(far, k), wz_recv.at[1, 3, k])
    arrived(g_slot.at[0:6], gz_send)
    for k in range(3):
        arrived(g_slot.at[0, 0], go_send.at[k])
    arrived(g_other.at[0:7], gx_send)
    arrived(g_relay, gr_send)
    arrived(g_relay, gf_send)
    arrived(x_slot.at[0:6], xz_send)
    arrived(x_relay, xr_send)
    arrived(x_relay, xf_send)
    arrived(x_all.at[:, 0], xo_send)
    arrived(x_all.at[:, 0:2], xp_send)
    arrived(g_all.at[0:7], ag_send)
    arrived(acc.at[0 : 3 * rows], half_send)
    arrived(norms.at[0 : ND - 1], norm_send)
    arrived(got.at[0 : 2 * (ND - 1)], bg_send)
    arrived(tag.at[0 : ND - 1], tag_send)
    arrived(slabs.at[0:7], wz_send)


def finish_kernel(owner, slots, new_w, new_m, new_t, out, w_out, m_out, t_out, sem):
    copies = [
        pltpu.make_async_copy(
            slots.at[owner[l], q],
            out.at[l, :, q * slots.shape[3] : (q + 1) * slots.shape[3]],
            sem.at[4 * l + q],
        )
        for l in range(NZ)
        for q in range(4)
    ] + [
        pltpu.make_async_copy(new_w, w_out, sem.at[4 * NZ]),
        pltpu.make_async_copy(new_m, m_out, sem.at[4 * NZ + 1]),
        pltpu.make_async_copy(new_t, t_out, sem.at[4 * NZ + 2]),
    ]
    for copy in copies:
        copy.start()
    for copy in copies:
        copy.wait()


def local(
    layer_inputs,
    output_grads,
    layer_owner,
    master_weights,
    momentum,
    table_blocks,
    block_grads,
    block_ids,
    block_counts,
):
    layers, tokens, rows = layer_inputs.shape
    per, cols = output_grads.shape[1:]
    quarter = cols // 4
    nb, tall, wide = table_blocks.shape[1:]
    f32, bf16, i32 = jnp.float32, jnp.bfloat16, jnp.int32
    hbm = pl.BlockSpec(memory_space=pltpu.HBM)
    smem = pl.BlockSpec(memory_space=pltpu.SMEM)
    anywhere = pl.BlockSpec(memory_space=pl.ANY)
    dma = pltpu.SemaphoreType.DMA
    slots, new_w, new_m, new_t = pl.pallas_call(
        step_kernel,
        name="step",
        out_shape=(
            pltpu.VMEM((NZ, 4, rows, quarter), bf16),
            pltpu.VMEM(master_weights.shape, f32),
            pltpu.VMEM(momentum.shape, f32),
            pltpu.VMEM(table_blocks.shape, f32),
        ),
        in_specs=[smem, smem, smem] + [hbm] * 6,
        out_specs=(pl.BlockSpec(memory_space=pltpu.VMEM),) * 4,
        scratch_shapes=[
            pltpu.VMEM((layers, tokens, rows), bf16),
            pltpu.VMEM((layers, tokens, rows), bf16),
            pltpu.VMEM((NZ, 4, tokens, rows), bf16),
            pltpu.VMEM((4 * rows, tokens // 2), bf16),
            pltpu.VMEM((2, 2, tokens // NY, rows), bf16),
            pltpu.VMEM((layers, per, cols), bf16),
            pltpu.VMEM((layers, 4, per, quarter), bf16),
            pltpu.VMEM((layers, 2, per, quarter), bf16),
            pltpu.VMEM((NZ, 2, 2, NX, 2 * per, quarter), bf16),
            pltpu.VMEM((2, 2, per, quarter), bf16),
            pltpu.VMEM((4 * rows, quarter), f32),
            pltpu.VMEM((rows, cols), f32),
            pltpu.VMEM((nb, tall, wide), f32),
            pltpu.VMEM((2 * ND, wide // nb, wide), bf16),
            pltpu.VMEM((wide, 2 * ND * (wide // nb)), bf16),
            pltpu.VMEM((2 * ND, tall, wide), bf16),
            pltpu.VMEM((ND, 8, wide), i32),
            pltpu.VMEM((ND, 8, wide), i32),
            pltpu.VMEM((ND, 2, 128), f32),
            dma((6,)),
            dma,
            dma((NZ,)),
            dma((3,)),
            dma,
            dma((NZ,)),
            dma,
            dma((2,)),
            dma,
            dma,
            dma((NZ, 2)),
            dma,
            dma((2, 2)),
            dma,
            dma,
            dma((NZ, 2)),
            dma,
            dma((NZ, 2)),
            dma,
            dma((NZ, 7)),
            dma,
            dma((3,)),
            dma,
            dma,
            dma,
            dma,
            dma,
            dma,
            dma,
            dma((2, 4, 4)),
        ],
        compiler_params=pltpu.CompilerParams(
            collective_id=0, has_side_effects=True, vmem_limit_bytes=60_160_000
        ),
    )(
        layer_owner,
        block_ids,
        block_counts,
        layer_inputs,
        output_grads,
        master_weights,
        momentum,
        table_blocks,
        block_grads,
    )
    new_weights, new_master, new_moment, new_table = pl.pallas_call(
        finish_kernel,
        name="finish",
        in_specs=[smem] + [anywhere] * 4,
        out_specs=(hbm,) * 4,
        scratch_shapes=[dma((4 * NZ + 3,))],
        out_shape=(
            jax.ShapeDtypeStruct((layers, rows, cols), bf16),
            jax.ShapeDtypeStruct(master_weights.shape, f32),
            jax.ShapeDtypeStruct(momentum.shape, f32),
            jax.ShapeDtypeStruct(table_blocks.shape, f32),
        ),
        compiler_params=pltpu.CompilerParams(vmem_limit_bytes=1024 * 1024),
    )(layer_owner, slots, new_w, new_m, new_t)
    return new_master, new_moment, new_weights, new_table


def solution(mesh):
    return jax.shard_map(
        local,
        mesh=mesh,
        in_specs=(
            P(None, "grp", "dev"),
            P(None, ("grp", "dev"), None),
            P(),
            P("grp", "dev", None),
            P("grp", "dev", None),
            P("grp", "dev", None, None),
            P("grp", "dev", None, None, None),
            P("grp", "dev", None),
            P("grp", "dev", None),
        ),
        out_specs=(
            P("grp", "dev", None),
            P("grp", "dev", None),
            P(None, "dev", None),
            P("grp", "dev", None, None),
        ),
        check_vma=False,
    )
```

```python
import functools

import jax
import jax.numpy as jnp
from jax import lax
from jax.experimental import pallas as pl
from jax.experimental.pallas import tpu as pltpu
from jax.sharding import PartitionSpec as P

tower_rate = 0.5
momentum_keep = 0.9
tower_decay = 0.1
table_rate = 0.5
table_decay = 0.2
eps_norm = 1e-06

NZ = 8
NX = 4
NY = 4
ND = NX * NY * 2


def step_kernel(
    owner,
    ids,
    counts,
    x_hbm,
    g_hbm,
    w_hbm,
    m_hbm,
    t_hbm,
    bg_hbm,
    slabs,
    w,
    m,
    table,
    x_in,
    x_slot,
    x_all,
    x_relay,
    g_in,
    g_slot,
    g_other,
    g_all,
    g_relay,
    acc,
    grad,
    sums,
    pick,
    turned,
    got,
    tag,
    got_tag,
    norms,
    in_sem,
    gz_send,
    gz_recv,
    go_send,
    gx_send,
    gx_recv,
    gr_send,
    gr_recv,
    gf_send,
    xz_send,
    xz_recv,
    xr_send,
    xr_recv,
    xf_send,
    xo_send,
    xo_recv,
    xp_send,
    xp_recv,
    ag_send,
    ag_recv,
    half_send,
    half_recv,
    norm_send,
    norm_recv,
    bg_send,
    bg_recv,
    tag_send,
    tag_recv,
    wz_send,
    wz_recv,
):
    z = lax.axis_index("grp")
    d = lax.axis_index("dev")
    core = d % 2
    cx = (d // 2) % NX
    cy = d // (2 * NX)
    chip = d // 2
    side = cy // 2
    duo = ((cy + 1) // 2) % 2
    oy = NY - 1 - cy
    iy = cy + 1 - 2 * (cy % 2)
    me = side * 2 + core
    pal = chip * 2 + 1 - core
    outer = (oy * NX + cx) * 2 + core
    inner = (iy * NX + cx) * 2 + core
    right = (cy * NX + (cx + 1) % NX) * 2 + core
    left = (cy * NX + (cx + NX - 1) % NX) * 2 + core
    rows = w_hbm.shape[1]
    cols = w_hbm.shape[2]
    quarter = cols // 4
    per = g_hbm.shape[1]
    tokens = x_hbm.shape[1]
    band = tokens // NY

    def send(src, dst, s_sem, r_sem, zz, dd):
        pltpu.make_async_remote_copy(
            src_ref=src,
            dst_ref=dst,
            send_sem=s_sem,
            recv_sem=r_sem,
            device_id=(zz, dd),
            device_id_type=pl.DeviceIdType.MESH,
        ).start()

    def arrived(ref, sem):
        pltpu.make_async_copy(ref, ref, sem).wait()

    def column(i):
        off = (i % 2) * ((i + 1) // 2) + (1 - i % 2) * (NZ - i // 2)
        return (z + off) % NZ

    g_load = pltpu.make_async_copy(g_hbm, g_in, in_sem.at[1])
    x_load = pltpu.make_async_copy(x_hbm, x_in, in_sem.at[0])
    w_load = pltpu.make_async_copy(w_hbm.at[0], w.at[0], in_sem.at[2])
    m_load = pltpu.make_async_copy(m_hbm.at[0], m.at[0], in_sem.at[3])
    t_load = pltpu.make_async_copy(t_hbm.at[0], table.at[0], in_sem.at[4])
    own_load = pltpu.make_async_copy(
        bg_hbm.at[0, 0, pl.ds(2 * d, 2)], got.at[pl.ds(2 * d, 2)], in_sem.at[5]
    )
    g_load.start()
    barrier = pltpu.get_barrier_semaphore()

    @pl.loop(1, ND)
    def _(p):
        pl.semaphore_signal(
            barrier, inc=1, device_id=(z, (d + p) % ND), device_id_type=pl.DeviceIdType.MESH
        )

    @pl.loop(1, NZ)
    def _(p):
        for cc in range(2):
            pl.semaphore_signal(
                barrier,
                inc=1,
                device_id=((z + p) % NZ, chip * 2 + cc),
                device_id_type=pl.DeviceIdType.MESH,
            )

    x_load.start()
    w_load.start()
    m_load.start()
    t_load.start()
    own_load.start()

    def layer_of(s):
        found = jnp.int32(0)
        for l in range(NZ):
            found = jnp.where(owner[l] == s, l, found)
        return found
    g_load.wait()

    @pl.loop(0, NZ)
    def _(s):
        l = layer_of(s)
        for q in range(4):
            g_slot[s, q] = g_in[l, :, q * quarter : (q + 1) * quarter]

    g_all[z, duo, side, cx, pl.ds(core * per, per), :] = g_slot[z, me]
    pl.semaphore_wait(barrier, ND - 1 + 2 * (NZ - 1))
    def g_home(zs):
        return g_all.at[zs, duo, side, cx, pl.ds(core * per, per)]

    far = (z + NZ // 2) % NZ
    ways = (1, NZ - 1)
    there = (1 - side) * 2 + core
    mine = pl.ds(2 * side, 2)
    theirs = pl.ds(2 * (1 - side), 2)

    def g_there(zs):
        return g_all.at[zs, duo, 1 - side, cx, pl.ds(core * per, per)]

    send(g_slot.at[z, side * 2 + 1 - core], g_home(z), go_send.at[0], gz_recv.at[z], z, pal)
    for cc in range(2):
        send(
            g_slot.at[z, (1 - side) * 2 + cc],
            g_home(z),
            go_send.at[1 + cc],
            gz_recv.at[z],
            z,
            (oy * NX + cx) * 2 + cc,
        )

    def g_cross(zt):
        send(g_slot.at[zt, theirs], g_other.at[zt], gx_send, gx_recv.at[zt], z, outer)

    g_cross((z + 1) % NZ)
    g_cross((z + NZ - 1) % NZ)
    g_cross(far)
    for j in (2, 3):
        g_cross((z + j) % NZ)
        g_cross((z + NZ - j) % NZ)

    send(g_slot.at[far, mine], g_relay.at[0], gr_send, gr_recv.at[0], (z + 1) % NZ, d)
    def g_own(j):
        for zt in ((z + j) % NZ, (z + NZ - j) % NZ):
            for cc in range(2):
                send(
                    g_slot.at[zt, 2 * side + cc],
                    g_home(z),
                    gz_send,
                    gz_recv.at[z],
                    zt,
                    chip * 2 + cc,
                )

    def g_for_other(j):
        for zt in ((z + j) % NZ, (z + NZ - j) % NZ):
            arrived(g_other.at[zt], gx_recv.at[zt])
            for cc in range(2):
                send(
                    g_other.at[zt, cc], g_there(z), gz_send, gz_recv.at[z], zt, chip * 2 + cc
                )

    def x_out(j):
        for h in range(2):
            for zt in ((z + j) % NZ, (z + NZ - j) % NZ):
                at = pl.ds(2 * h, 2)
                send(
                    x_slot.at[zt, at], x_all.at[z, me, at], xz_send, xz_recv.at[z, h], zt, d
                )

    def x_half(zs, s, h):
        return x_all.at[zs, s, pl.ds(2 * h, 2)]

    def x_share(zs, h):
        ref = x_half(zs, me, h)
        send(ref, ref, xo_send, xo_recv.at[zs, h], z, outer)
        send(ref, ref, xp_send, xp_recv.at[zs, h], z, pal)

    def x_first(j, h):
        for zs in ((z + j) % NZ, (z + NZ - j) % NZ):
            arrived(x_half(zs, me, h), xz_recv.at[zs, h])
            x_share(zs, h)

    def x_first_far(h):
        arrived(x_half(far, me, h), xz_recv.at[far, h])
        x_share(far, h)

    def x_second(zs, h):
        ref = x_half(zs, there, h)
        arrived(ref, xo_recv.at[zs, h])
        send(ref, ref, xp_send, xp_recv.at[zs, h], z, pal)

    def x_second_both(j, h):
        for zs in ((z + j) % NZ, (z + NZ - j) % NZ):
            x_second(zs, h)

    g_own(1)
    g_own(2)

    x_load.wait()

    @pl.loop(0, NZ)
    def _(s):
        l = layer_of(s)
        for y in range(NY):
            x_slot[s, y] = x_in[l, y * band : (y + 1) * band, :].T

    x_all[z, me] = x_slot[z]

    for way in range(2):
        for h in range(2):
            send(
                x_slot.at[far, 2 * h + way],
                x_relay.at[way, h],
                xr_send,
                xr_recv.at[way, h],
                (z + ways[way]) % NZ,
                d,
            )

    for h in range(2):
        x_share(z, h)

    def whole(zs, pr, da):
        return g_all.at[zs, pr, :, (cx + da + NX) % NX]

    def part(zs, pr, da, h):
        return g_all.at[zs, pr, h, (cx + da + NX) % NX]

    def push(ref, zs, k, dd):
        send(ref, ref, ag_send, ag_recv.at[zs, k], z, dd)

    def landed(it):
        zs = column(it)

        @pl.when(it == 0)
        def _():
            arrived(g_slot.at[0, 0:3], gz_recv.at[zs])

        @pl.when(it > 0)
        def _():
            arrived(g_slot.at[0], gz_recv.at[zs])

    def feed(it):
        @pl.when(it == 0)
        def _():
            g_for_other(1)
            x_out(1)
            arrived(g_other.at[far], gx_recv.at[far])
            send(g_other.at[far], g_relay.at[1], gr_send, gr_recv.at[1], (z + NZ - 1) % NZ, d)

        @pl.when(it == 1)
        def _():
            g_for_other(2)
            g_own(3)
            g_for_other(3)
            x_out(2)

        @pl.when(it == 2)
        def _():
            relay()

    def relay():
        for way in range(2):
            zs = (z + NZ - ways[way]) % NZ
            zt = (zs + NZ // 2) % NZ
            arrived(g_relay.at[way], gr_recv.at[way])
            home = g_home(zs) if way == 0 else g_there(zs)
            sem = gz_recv.at[zs]
            for cc in range(2):
                send(g_relay.at[way, cc], home, gf_send, sem, zt, chip * 2 + cc)

        x_out(3)
        for way in range(2):
            zs = (z + NZ - ways[way]) % NZ
            zt = (zs + NZ // 2) % NZ
            for h in range(2):
                arrived(x_relay.at[way, h], xr_recv.at[way, h])
                send(
                    x_relay.at[way, h],
                    x_all.at[zs, me, 2 * h + way],
                    xf_send,
                    xz_recv.at[zs, h],
                    zt,
                    d,
                )

    def multiply(u):
        k = u // 2
        h = u % 2
        zs = column(k)
        arrived(x_slot.at[0], xp_recv.at[zs, h])
        @pl.loop(0, quarter // 256)
        def _(n):
            where = pl.ds(pl.multiple_of(n * 256, 256), 256)
            total = acc[:, where]
            for pr in range(2):
                y = pr + h * (NY - 1 - 2 * pr)
                total = total + jnp.dot(
                    x_all[zs, :, y].reshape(4 * rows, band),
                    g_all[zs, pr, h, :, :, where].reshape(band, 256),
                    preferred_element_type=jnp.float32,
                )
            acc[:, where] = total

    def x_stages(it):
        @pl.when(it == 2)
        def _():
            for h in range(2):
                x_second(z, h)

        def event(steps, do):
            for when, *what in steps:

                @pl.when(it == when)
                def _():
                    do(*what)

        event(
            ((3, 1, 0), (4, 1, 1), (5, 2, 0), (6, 2, 1), (8, 3, 0), (9, 3, 1)),
            x_first,
        )
        event(
            ((5, 1, 0), (6, 1, 1), (7, 2, 0), (8, 2, 1), (10, 3, 0), (11, 3, 1)),
            x_second_both,
        )
        event(((10, 0), (10, 1)), x_first_far)
        event(((12, far, 0), (13, far, 1)), x_second)

        first = jnp.where(
            it < 7, 0, jnp.where(it < 12, 2 * it - 12, it + 1)
        )
        count = jnp.where(
            it == 11, 3, jnp.where(it == 12, 1, jnp.where((it == 4) | (it >= 7), 2, 0))
        )

        @pl.loop(first, first + count)
        def _(v):
            multiply(v + jnp.where(v == 11, 1, 0) - jnp.where(v == 12, 1, 0))
    @pl.loop(0, ND)
    def _(j):
        for r in range(2):
            t = jnp.where(r < counts[0, 0, j], ids[0, 0, 2 * j + r], -1)
            tag[j, r : r + 1, :] = jnp.full((1, tag.shape[2]), t, jnp.int32)

    got_tag[d] = tag[d]
    acc[...] = jnp.zeros_like(acc)
    w_load.wait()

    def weight_step(i, total):
        v = w[0, pl.ds(pl.multiple_of(i * 8, 8), 8), :]
        v = v * v
        for k in range(cols // 128):
            total = total + v[:, k * 128 : (k + 1) * 128]
        return total

    weight_sq = lax.fori_loop(0, rows // 8, weight_step, jnp.zeros((8, 128), jnp.float32))
    @pl.when(core == 0)
    def _():
        @pl.loop(0, NZ + 6)
        def _(it):
            @pl.when(it < NZ)
            def _():
                zs = column(it)
                landed(it)
                push(whole(zs, duo, 0), zs, 0, right)
                push(whole(zs, duo, 0), zs, 1, left)
                push(whole(zs, duo, 0), zs, 3, inner)

            @pl.when((it >= 1) & (it < NZ + 1))
            def _():
                zs = column(it - 1)
                arrived(whole(zs, duo, -1), ag_recv.at[zs, 0])
                push(part(zs, duo, -1, 0), zs, 2, right)
                push(whole(zs, duo, -1), zs, 3, inner)
                arrived(whole(zs, duo, 1), ag_recv.at[zs, 1])
                push(part(zs, duo, 1, 1), zs, 2, left)
                push(whole(zs, duo, 1), zs, 3, inner)

            feed(it)

            @pl.when((it >= 2) & (it < NZ + 2))
            def _():
                zs = column(it - 2)
                arrived(whole(zs, duo, 2), ag_recv.at[zs, 2])
                push(whole(zs, duo, 2), zs, 3, inner)

            @pl.when((it >= 3) & (it < NZ + 3))
            def _():
                zs = column(it - 3)
                arrived(g_all.at[zs, 1 - duo], ag_recv.at[zs, 3])

            x_stages(it)

    @pl.when(core == 1)
    def _():
        @pl.loop(0, NZ + 6)
        def _(it):
            @pl.when(it < NZ)
            def _():
                zs = column(it)
                landed(it)
                push(whole(zs, duo, 0), zs, 3, inner)
                push(whole(zs, duo, 0), zs, 0, right)
                push(whole(zs, duo, 0), zs, 1, left)

            @pl.when((it >= 1) & (it < NZ + 1))
            def _():
                zs = column(it - 1)
                arrived(whole(zs, 1 - duo, 0), ag_recv.at[zs, 3])
                push(whole(zs, 1 - duo, 0), zs, 4, right)
                push(whole(zs, 1 - duo, 0), zs, 5, left)
                arrived(whole(zs, duo, -1), ag_recv.at[zs, 0])
                push(part(zs, duo, -1, 0), zs, 2, right)
                arrived(whole(zs, duo, 1), ag_recv.at[zs, 1])
                push(part(zs, duo, 1, 1), zs, 2, left)

            feed(it)

            @pl.when((it >= 2) & (it < NZ + 2))
            def _():
                zs = column(it - 2)
                arrived(whole(zs, 1 - duo, -1), ag_recv.at[zs, 4])
                push(part(zs, 1 - duo, -1, 0), zs, 6, right)
                arrived(whole(zs, 1 - duo, 1), ag_recv.at[zs, 5])
                push(part(zs, 1 - duo, 1, 1), zs, 6, left)
                arrived(whole(zs, duo, 2), ag_recv.at[zs, 2])

            @pl.when((it >= 3) & (it < NZ + 3))
            def _():
                zs = column(it - 3)
                arrived(whole(zs, 1 - duo, 2), ag_recv.at[zs, 6])

            x_stages(it)
    def grad_step(i, total):
        for k in range(4):
            v = acc[pl.ds(pl.multiple_of(i * 32 + k * 8, 8), 8), :]
            total = total + v * v
        return total

    wide_sq = lax.fori_loop(0, 4 * rows // 32, grad_step, jnp.zeros((8, quarter), jnp.float32))
    grad_sq = wide_sq[:, 0:128]
    for k in range(1, quarter // 128):
        grad_sq = grad_sq + wide_sq[:, k * 128 : (k + 1) * 128]
    norms[d, 0:1] = jnp.sum(weight_sq, axis=0, keepdims=True)
    norms[d, 1:2] = jnp.sum(grad_sq, axis=0, keepdims=True)
    grad[:, pl.ds(pl.multiple_of(me * quarter, quarter), quarter)] = acc[pl.ds(me * rows, rows), :]

    @pl.loop(1, ND)
    def _(p):
        send(norms.at[d], norms.at[d], norm_send, norm_recv, z, (d + p) % ND)
    mates = (
        (me, d),
        (side * 2 + 1 - core, pal),
        ((1 - side) * 2 + core, outer),
        ((1 - side) * 2 + 1 - core, outer + 1 - 2 * core),
    )

    def columns(k):
        return pl.ds(pl.multiple_of(mates[k][0] * quarter, quarter), quarter)

    for k in range(1, 4):
        send(
            acc.at[pl.ds(mates[k][0] * rows, rows)],
            grad.at[:, columns(0)],
            half_send,
            half_recv.at[k - 1],
            z,
            mates[k][1],
        )

    def block_out(j):
        send(tag.at[j], got_tag.at[d], tag_send, tag_recv, z, j)
        send(
            bg_hbm.at[0, 0, pl.ds(2 * j, 2)],
            got.at[pl.ds(2 * d, 2)],
            bg_send,
            bg_recv,
            z,
            j,
        )

    near = ND // 2
    m_load.wait()

    arrived(norms.at[0 : ND - 1], norm_recv)
    totals = jnp.sum(norms[...], axis=0)
    weight_total = jnp.sum(totals[0:1], keepdims=True)
    grad_total = jnp.sum(totals[1:2], keepdims=True)
    weight_norm = jnp.sqrt(weight_total + eps_norm)
    trust = weight_norm / (jnp.sqrt(grad_total + eps_norm) + tower_decay * weight_norm)
    scale = tower_rate * trust

    strip = 16
    up = (z + 1) % NZ
    down = (z + NZ - 1) % NZ

    cut = rows // 2

    def piece(s, k, r):
        return slabs.at[s, mates[k][0], pl.ds(r * cut, cut)]

    def pass_on(s, k, r, way, hop):
        send(
            piece(s, k, r),
            piece(s, k, r),
            wz_send,
            wz_recv.at[way, hop, 2 * k + r],
            (up, down)[way],
            d,
        )

    def came(s, k, r, way, hop):
        arrived(piece(s, k, r), wz_recv.at[way, hop, 2 * k + r])

    def renew(k):
        for r in range(2):

            @pl.loop(0, cut // strip)
            def _(i):
                at = pl.ds(pl.multiple_of(r * cut + i * strip, strip), strip)
                old = w[0, at, columns(k)]
                new_m = momentum_keep * m[0, at, columns(k)] + scale * (
                    grad[at, columns(k)] + tower_decay * old
                )
                new_w = old - new_m
                m[0, at, columns(k)] = new_m
                w[0, at, columns(k)] = new_w
                slabs[z, mates[k][0], at, :] = new_w.astype(jnp.bfloat16)

            for way in range(2):
                pass_on(z, k, r, way, 0)

    def onward(j, ks):
        for k in ks:
            for r in range(2):
                for way in range(2):
                    if j < 3 or k % 2 == way:
                        s = ((z + NZ - j) % NZ, (z + j) % NZ)[way]
                        came(s, k, r, way, j - 1)
                        pass_on(s, k, r, way, j)
    renew(0)
    arrived(grad.at[:, columns(1)], half_recv.at[0])
    renew(1)

    @pl.loop(1, near)
    def _(p):
        block_out(side * near + (d + p) % near)
    onward(1, (0,))
    arrived(grad.at[:, columns(2)], half_recv.at[1])
    renew(2)
    onward(1, (1,))
    onward(2, (0,))
    arrived(grad.at[:, columns(3)], half_recv.at[2])
    renew(3)
    @pl.loop(0, near)
    def _(p):
        block_out((1 - side) * near + (d + p) % near)
    onward(2, (1,))
    onward(1, (2, 3))
    onward(3, (0, 1))
    onward(2, (2, 3))
    onward(3, (2, 3))
    own_load.wait()
    t_load.wait()

    arrived(got.at[0 : 2 * (ND - 1)], bg_recv)
    arrived(got_tag.at[0 : ND - 1], tag_recv)
    nb = table.shape[1]
    wide = table.shape[3]
    lane = lax.broadcasted_iota(jnp.int32, (strip, wide), 1)
    same = lane % strip == lax.broadcasted_iota(jnp.int32, (strip, wide), 0)
    names = lane // strip

    @pl.loop(0, ND)
    def _(s):
        for r in range(2):
            hit = (got_tag[s, r : r + 1, :] == names) & same
            pick[2 * s + r] = jnp.where(hit, 1.0, 0.0).astype(jnp.bfloat16)

    turned[...] = pick[...].reshape(2 * ND * strip, wide).T

    @pl.loop(0, table.shape[2] // strip)
    def _(i):
        at = pl.ds(pl.multiple_of(i * strip, strip), strip)
        values = got[:, at, :].reshape(2 * ND * strip, wide)
        total = jnp.dot(turned[...], values, preferred_element_type=jnp.float32)
        sums[:, at, :] = total.reshape(nb, strip, wide)

    tags = got_tag[:, 0:2, :]
    for b in range(nb):
        hits = jnp.sum(jnp.where(tags == b, 1.0, 0.0), axis=(0, 1)).reshape(1, wide)
        flat = table[0, b]
        total = sums[b]
        w_norm = jnp.sqrt(jnp.sum(flat * flat, keepdims=True) + eps_norm)
        g_norm = jnp.sqrt(jnp.sum(total * total, keepdims=True) + eps_norm)
        block_trust = w_norm / (g_norm + table_decay * w_norm)
        moved = flat - table_rate * block_trust * (total + table_decay * flat)
        table[0, b] = jnp.where(hits > 0, moved, flat)
    for k in range(4):
        way = k % 2
        for r in range(2):
            came(((z + 3) % NZ, (z + NZ - 3) % NZ)[way], k, r, 1 - way, 2)
            came(far, k, r, way, 3)
    arrived(g_slot.at[0:6], gz_send)
    for k in range(3):
        arrived(g_slot.at[0, 0], go_send.at[k])
    arrived(g_other.at[0:7], gx_send)
    arrived(g_relay, gr_send)
    arrived(g_relay, gf_send)
    arrived(x_slot.at[0:6], xz_send)
    arrived(x_relay, xr_send)
    arrived(x_relay, xf_send)
    arrived(x_all.at[:, 0], xo_send)
    arrived(x_all.at[:, 0:2], xp_send)
    arrived(g_all.at[0:7], ag_send)
    arrived(acc.at[0 : 3 * rows], half_send)
    arrived(norms.at[0 : ND - 1], norm_send)
    arrived(got.at[0 : 2 * (ND - 1)], bg_send)
    arrived(tag.at[0 : ND - 1], tag_send)
    arrived(slabs.at[0:7], wz_send)


def finish_kernel(owner, slots, new_w, new_m, new_t, out, w_out, m_out, t_out, sem):
    copies = [
        pltpu.make_async_copy(
            slots.at[owner[l], q],
            out.at[l, :, q * slots.shape[3] : (q + 1) * slots.shape[3]],
            sem.at[4 * l + q],
        )
        for l in range(NZ)
        for q in range(4)
    ] + [
        pltpu.make_async_copy(new_w, w_out, sem.at[4 * NZ]),
        pltpu.make_async_copy(new_m, m_out, sem.at[4 * NZ + 1]),
        pltpu.make_async_copy(new_t, t_out, sem.at[4 * NZ + 2]),
    ]
    for copy in copies:
        copy.start()
    for copy in copies:
        copy.wait()


def local(
    layer_inputs,
    output_grads,
    layer_owner,
    master_weights,
    momentum,
    table_blocks,
    block_grads,
    block_ids,
    block_counts,
):
    layers, tokens, rows = layer_inputs.shape
    per, cols = output_grads.shape[1:]
    quarter = cols // 4
    nb, tall, wide = table_blocks.shape[1:]
    f32, bf16, i32 = jnp.float32, jnp.bfloat16, jnp.int32
    hbm = pl.BlockSpec(memory_space=pltpu.HBM)
    smem = pl.BlockSpec(memory_space=pltpu.SMEM)
    anywhere = pl.BlockSpec(memory_space=pl.ANY)
    dma = pltpu.SemaphoreType.DMA
    slots, new_w, new_m, new_t = pl.pallas_call(
        step_kernel,
        name="step",
        out_shape=(
            pltpu.VMEM((NZ, 4, rows, quarter), bf16),
            pltpu.VMEM(master_weights.shape, f32),
            pltpu.VMEM(momentum.shape, f32),
            pltpu.VMEM(table_blocks.shape, f32),
        ),
        in_specs=[smem, smem, smem] + [hbm] * 6,
        out_specs=(pl.BlockSpec(memory_space=pltpu.VMEM),) * 4,
        scratch_shapes=[
            pltpu.VMEM((layers, tokens, rows), bf16),
            pltpu.VMEM((layers, NY, rows, tokens // NY), bf16),
            pltpu.VMEM((NZ, 4, NY, rows, tokens // NY), bf16),
            pltpu.VMEM((2, 2, rows, tokens // NY), bf16),
            pltpu.VMEM((layers, per, cols), bf16),
            pltpu.VMEM((layers, 4, per, quarter), bf16),
            pltpu.VMEM((layers, 2, per, quarter), bf16),
            pltpu.VMEM((NZ, 2, 2, NX, 2 * per, quarter), bf16),
            pltpu.VMEM((2, 2, per, quarter), bf16),
            pltpu.VMEM((4 * rows, quarter), f32),
            pltpu.VMEM((rows, cols), f32),
            pltpu.VMEM((nb, tall, wide), f32),
            pltpu.VMEM((2 * ND, wide // nb, wide), bf16),
            pltpu.VMEM((wide, 2 * ND * (wide // nb)), bf16),
            pltpu.VMEM((2 * ND, tall, wide), bf16),
            pltpu.VMEM((ND, 8, wide), i32),
            pltpu.VMEM((ND, 8, wide), i32),
            pltpu.VMEM((ND, 2, 128), f32),
            dma((6,)),
            dma,
            dma((NZ,)),
            dma((3,)),
            dma,
            dma((NZ,)),
            dma,
            dma((2,)),
            dma,
            dma,
            dma((NZ, 2)),
            dma,
            dma((2, 2)),
            dma,
            dma,
            dma((NZ, 2)),
            dma,
            dma((NZ, 2)),
            dma,
            dma((NZ, 7)),
            dma,
            dma((3,)),
            dma,
            dma,
            dma,
            dma,
            dma,
            dma,
            dma,
            dma((2, 4, 8)),
        ],
        compiler_params=pltpu.CompilerParams(
            collective_id=0, has_side_effects=True, vmem_limit_bytes=60_160_000
        ),
    )(
        layer_owner,
        block_ids,
        block_counts,
        layer_inputs,
        output_grads,
        master_weights,
        momentum,
        table_blocks,
        block_grads,
    )
    new_weights, new_master, new_moment, new_table = pl.pallas_call(
        finish_kernel,
        name="finish",
        in_specs=[smem] + [anywhere] * 4,
        out_specs=(hbm,) * 4,
        scratch_shapes=[dma((4 * NZ + 3,))],
        out_shape=(
            jax.ShapeDtypeStruct((layers, rows, cols), bf16),
            jax.ShapeDtypeStruct(master_weights.shape, f32),
            jax.ShapeDtypeStruct(momentum.shape, f32),
            jax.ShapeDtypeStruct(table_blocks.shape, f32),
        ),
        compiler_params=pltpu.CompilerParams(vmem_limit_bytes=1024 * 1024),
    )(layer_owner, slots, new_w, new_m, new_t)
    return new_master, new_moment, new_weights, new_table


def solution(mesh):
    return jax.shard_map(
        local,
        mesh=mesh,
        in_specs=(
            P(None, "grp", "dev"),
            P(None, ("grp", "dev"), None),
            P(),
            P("grp", "dev", None),
            P("grp", "dev", None),
            P("grp", "dev", None, None),
            P("grp", "dev", None, None, None),
            P("grp", "dev", None),
            P("grp", "dev", None),
        ),
        out_specs=(
            P("grp", "dev", None),
            P("grp", "dev", None),
            P(None, "dev", None),
            P("grp", "dev", None, None),
        ),
        check_vma=False,
    )
```

```python
import functools

import jax
import jax.numpy as jnp
from jax import lax
from jax.experimental import pallas as pl
from jax.experimental.pallas import tpu as pltpu
from jax.sharding import PartitionSpec as P

tower_rate = 0.5
momentum_keep = 0.9
tower_decay = 0.1
table_rate = 0.5
table_decay = 0.2
eps_norm = 1e-06

NZ = 8
NX = 4
NY = 4
ND = NX * NY * 2


def step_kernel(
    owner_hbm,
    ids_hbm,
    counts_hbm,
    x_hbm,
    g_hbm,
    w_hbm,
    m_hbm,
    t_hbm,
    bg_hbm,
    slabs,
    w,
    m,
    table,
    x_in,
    x_slot,
    x_all,
    x_relay,
    g_in,
    g_slot,
    g_other,
    g_all,
    g_relay,
    acc,
    grad,
    sums,
    pick,
    turned,
    got,
    tag,
    got_tag,
    norms,
    grad_sq,
    owner,
    ids,
    counts,
    in_sem,
    gz_send,
    gz_recv,
    go_send,
    gx_send,
    gx_recv,
    gr_send,
    gr_recv,
    gf_send,
    xz_send,
    xz_recv,
    xr_send,
    xr_recv,
    xf_send,
    xo_send,
    xo_recv,
    xp_send,
    xp_recv,
    ag_send,
    ag_recv,
    half_send,
    half_recv,
    norm_send,
    norm_recv,
    bg_send,
    bg_recv,
    tag_send,
    tag_recv,
    wz_send,
    wz_recv,
):
    z = lax.axis_index("grp")
    d = lax.axis_index("dev")
    core = d % 2
    cx = (d // 2) % NX
    cy = d // (2 * NX)
    chip = d // 2
    side = cy // 2
    duo = ((cy + 1) // 2) % 2
    oy = NY - 1 - cy
    iy = cy + 1 - 2 * (cy % 2)
    me = side * 2 + core
    pal = chip * 2 + 1 - core
    outer = (oy * NX + cx) * 2 + core
    inner = (iy * NX + cx) * 2 + core
    right = (cy * NX + (cx + 1) % NX) * 2 + core
    left = (cy * NX + (cx + NX - 1) % NX) * 2 + core
    rows = w_hbm.shape[1]
    cols = w_hbm.shape[2]
    quarter = cols // 4
    per = g_hbm.shape[1]
    tokens = x_hbm.shape[1]
    band = tokens // NY

    def send(src, dst, s_sem, r_sem, zz, dd):
        pltpu.make_async_remote_copy(
            src_ref=src,
            dst_ref=dst,
            send_sem=s_sem,
            recv_sem=r_sem,
            device_id=(zz, dd),
            device_id_type=pl.DeviceIdType.MESH,
        ).start()

    def arrived(ref, sem):
        pltpu.make_async_copy(ref, ref, sem).wait()

    def column(i):
        off = (i % 2) * ((i + 1) // 2) + (1 - i % 2) * (NZ - i // 2)
        return (z + off) % NZ

    g_load = pltpu.make_async_copy(g_hbm, g_in, in_sem.at[1])
    x_load = pltpu.make_async_copy(x_hbm, x_in, in_sem.at[0])
    w_load = pltpu.make_async_copy(w_hbm.at[0], w.at[0], in_sem.at[2])
    m_load = pltpu.make_async_copy(m_hbm.at[0], m.at[0], in_sem.at[3])
    t_load = pltpu.make_async_copy(t_hbm.at[0], table.at[0], in_sem.at[4])
    own_load = pltpu.make_async_copy(
        bg_hbm.at[0, 0, pl.ds(2 * d, 2)], got.at[pl.ds(2 * d, 2)], in_sem.at[5]
    )
    owner_load = pltpu.make_async_copy(owner_hbm, owner, in_sem.at[6])
    ids_load = pltpu.make_async_copy(ids_hbm, ids, in_sem.at[7])
    counts_load = pltpu.make_async_copy(counts_hbm, counts, in_sem.at[8])
    owner_load.start()
    g_load.start()
    barrier = pltpu.get_barrier_semaphore()

    @pl.loop(1, ND)
    def _(p):
        pl.semaphore_signal(
            barrier, inc=1, device_id=(z, (d + p) % ND), device_id_type=pl.DeviceIdType.MESH
        )

    @pl.loop(1, NZ)
    def _(p):
        for cc in range(2):
            pl.semaphore_signal(
                barrier,
                inc=1,
                device_id=((z + p) % NZ, chip * 2 + cc),
                device_id_type=pl.DeviceIdType.MESH,
            )

    x_load.start()
    w_load.start()
    m_load.start()
    t_load.start()
    own_load.start()
    ids_load.start()
    counts_load.start()

    def layer_of(s):
        found = jnp.int32(0)
        for l in range(NZ):
            found = jnp.where(owner[l] == s, l, found)
        return found
    owner_load.wait()
    g_load.wait()

    @pl.loop(0, NZ)
    def _(s):
        l = layer_of(s)
        for q in range(4):
            g_slot[s, q] = g_in[l, :, q * quarter : (q + 1) * quarter]

    g_all[z, duo, side, cx, pl.ds(core * per, per), :] = g_slot[z, me]
    pl.semaphore_wait(barrier, ND - 1 + 2 * (NZ - 1))
    def g_home(zs):
        return g_all.at[zs, duo, side, cx, pl.ds(core * per, per)]

    far = (z + NZ // 2) % NZ
    ways = (1, NZ - 1)
    there = (1 - side) * 2 + core
    mine = pl.ds(2 * side, 2)
    theirs = pl.ds(2 * (1 - side), 2)

    def g_there(zs):
        return g_all.at[zs, duo, 1 - side, cx, pl.ds(core * per, per)]

    send(g_slot.at[z, side * 2 + 1 - core], g_home(z), go_send.at[0], gz_recv.at[z], z, pal)
    for cc in range(2):
        send(
            g_slot.at[z, (1 - side) * 2 + cc],
            g_home(z),
            go_send.at[1 + cc],
            gz_recv.at[z],
            z,
            (oy * NX + cx) * 2 + cc,
        )

    def g_cross(zt):
        send(g_slot.at[zt, theirs], g_other.at[zt], gx_send, gx_recv.at[zt], z, outer)

    g_cross((z + 1) % NZ)
    g_cross((z + NZ - 1) % NZ)
    g_cross(far)
    for j in (2, 3):
        g_cross((z + j) % NZ)
        g_cross((z + NZ - j) % NZ)

    send(g_slot.at[far, mine], g_relay.at[0], gr_send, gr_recv.at[0], (z + 1) % NZ, d)
    def g_own(j):
        for zt in ((z + j) % NZ, (z + NZ - j) % NZ):
            for cc in range(2):
                send(
                    g_slot.at[zt, 2 * side + cc],
                    g_home(z),
                    gz_send,
                    gz_recv.at[z],
                    zt,
                    chip * 2 + cc,
                )

    def g_for_other(j):
        for zt in ((z + j) % NZ, (z + NZ - j) % NZ):
            arrived(g_other.at[zt], gx_recv.at[zt])
            for cc in range(2):
                send(
                    g_other.at[zt, cc], g_there(z), gz_send, gz_recv.at[z], zt, chip * 2 + cc
                )

    def x_out(j):
        for h in range(2):
            for zt in ((z + j) % NZ, (z + NZ - j) % NZ):
                at = pl.ds(2 * h, 2)
                send(
                    x_slot.at[zt, at], x_all.at[z, me, at], xz_send, xz_recv.at[z, h], zt, d
                )

    def x_half(zs, s, h):
        return x_all.at[zs, s, pl.ds(2 * h, 2)]

    def x_share(zs, h):
        ref = x_half(zs, me, h)
        send(ref, ref, xo_send, xo_recv.at[zs, h], z, outer)
        send(ref, ref, xp_send, xp_recv.at[zs, h], z, pal)

    def x_first(j, h):
        for zs in ((z + j) % NZ, (z + NZ - j) % NZ):
            arrived(x_half(zs, me, h), xz_recv.at[zs, h])
            x_share(zs, h)

    def x_first_far(h):
        arrived(x_half(far, me, h), xz_recv.at[far, h])
        x_share(far, h)

    def x_second(zs, h):
        ref = x_half(zs, there, h)
        arrived(ref, xo_recv.at[zs, h])
        send(ref, ref, xp_send, xp_recv.at[zs, h], z, pal)

    def x_second_both(j, h):
        for zs in ((z + j) % NZ, (z + NZ - j) % NZ):
            x_second(zs, h)

    g_own(1)
    g_own(2)

    x_load.wait()

    @pl.loop(0, NZ)
    def _(s):
        l = layer_of(s)
        for y in range(NY):
            x_slot[s, y] = x_in[l, y * band : (y + 1) * band, :].T

    x_all[z, me] = x_slot[z]

    for way in range(2):
        for h in range(2):
            send(
                x_slot.at[far, 2 * h + way],
                x_relay.at[way, h],
                xr_send,
                xr_recv.at[way, h],
                (z + ways[way]) % NZ,
                d,
            )

    for h in range(2):
        x_share(z, h)

    def whole(zs, pr, da):
        return g_all.at[zs, pr, :, (cx + da + NX) % NX]

    def part(zs, pr, da, h):
        return g_all.at[zs, pr, h, (cx + da + NX) % NX]

    def push(ref, zs, k, dd):
        send(ref, ref, ag_send, ag_recv.at[zs, k], z, dd)

    def landed(it):
        zs = column(it)

        @pl.when(it == 0)
        def _():
            arrived(g_slot.at[0, 0:3], gz_recv.at[zs])

        @pl.when(it > 0)
        def _():
            arrived(g_slot.at[0], gz_recv.at[zs])

    def feed(it):
        @pl.when(it == 0)
        def _():
            g_for_other(1)
            x_out(1)
            arrived(g_other.at[far], gx_recv.at[far])
            send(g_other.at[far], g_relay.at[1], gr_send, gr_recv.at[1], (z + NZ - 1) % NZ, d)

        @pl.when(it == 1)
        def _():
            g_for_other(2)
            g_own(3)
            g_for_other(3)
            x_out(2)

        @pl.when(it == 2)
        def _():
            relay()

    def relay():
        for way in range(2):
            zs = (z + NZ - ways[way]) % NZ
            zt = (zs + NZ // 2) % NZ
            arrived(g_relay.at[way], gr_recv.at[way])
            home = g_home(zs) if way == 0 else g_there(zs)
            sem = gz_recv.at[zs]
            for cc in range(2):
                send(g_relay.at[way, cc], home, gf_send, sem, zt, chip * 2 + cc)

        x_out(3)
        for way in range(2):
            zs = (z + NZ - ways[way]) % NZ
            zt = (zs + NZ // 2) % NZ
            for h in range(2):
                arrived(x_relay.at[way, h], xr_recv.at[way, h])
                send(
                    x_relay.at[way, h],
                    x_all.at[zs, me, 2 * h + way],
                    xf_send,
                    xz_recv.at[zs, h],
                    zt,
                    d,
                )

    def multiply(u, final=False):
        k = u // 2
        h = u % 2
        zs = column(k)
        arrived(x_slot.at[0], xp_recv.at[zs, h])
        @pl.loop(0, quarter // 256)
        def _(n):
            where = pl.ds(pl.multiple_of(n * 256, 256), 256)
            total = acc[:, where]
            for pr in range(2):
                y = pr + h * (NY - 1 - 2 * pr)
                total = total + jnp.dot(
                    x_all[zs, :, y].reshape(4 * rows, band),
                    g_all[zs, pr, h, :, :, where].reshape(band, 256),
                    preferred_element_type=jnp.float32,
                )
            acc[:, where] = total
            if final:
                squares = jnp.sum((total * total).reshape(4 * rows // 8, 8, 256), axis=0)
                grad_sq[...] += squares[:, :128] + squares[:, 128:]

    def x_stages(it):
        @pl.when(it == 2)
        def _():
            for h in range(2):
                x_second(z, h)

        def event(steps, do):
            for when, *what in steps:

                @pl.when(it == when)
                def _():
                    do(*what)

        event(
            ((3, 1, 0), (4, 1, 1), (5, 2, 0), (6, 2, 1), (8, 3, 0), (9, 3, 1)),
            x_first,
        )
        event(
            ((5, 1, 0), (6, 1, 1), (7, 2, 0), (8, 2, 1), (10, 3, 0), (11, 3, 1)),
            x_second_both,
        )
        event(((10, 0), (10, 1)), x_first_far)
        event(((12, far, 0), (13, far, 1)), x_second)

        first = jnp.where(
            it < 7, 0, jnp.where(it < 12, 2 * it - 12, it + 1)
        )
        count = jnp.where(
            it == 11, 3, jnp.where(it >= 12, 1, jnp.where((it == 4) | (it >= 7), 2, 0))
        )

        @pl.loop(first, first + count)
        def _(v):
            multiply(v + jnp.where(v == 11, 1, 0) - jnp.where(v == 12, 1, 0))
    ids_load.wait()
    counts_load.wait()

    @pl.loop(0, ND)
    def _(j):
        for r in range(2):
            t = jnp.where(r < counts[0, 0, j], ids[0, 0, 2 * j + r], -1)
            tag[j, r : r + 1, :] = jnp.full((1, tag.shape[2]), t, jnp.int32)

    got_tag[d] = tag[d]
    acc[...] = jnp.zeros_like(acc)
    w_load.wait()

    def weight_step(i, total):
        v = w[0, pl.ds(pl.multiple_of(i * 8, 8), 8), :]
        v = v * v
        for k in range(cols // 128):
            total = total + v[:, k * 128 : (k + 1) * 128]
        return total

    weight_sq = lax.fori_loop(0, rows // 8, weight_step, jnp.zeros((8, 128), jnp.float32))
    norms[d, 0:1] = jnp.sum(weight_sq, axis=0, keepdims=True)
    grad_sq[...] = jnp.zeros_like(grad_sq)
    @pl.when(core == 0)
    def _():
        @pl.loop(0, NZ + 6)
        def _(it):
            @pl.when(it < NZ)
            def _():
                zs = column(it)
                landed(it)
                push(whole(zs, duo, 0), zs, 0, right)
                push(whole(zs, duo, 0), zs, 1, left)
                push(whole(zs, duo, 0), zs, 3, inner)

            @pl.when((it >= 1) & (it < NZ + 1))
            def _():
                zs = column(it - 1)
                arrived(whole(zs, duo, -1), ag_recv.at[zs, 0])
                push(part(zs, duo, -1, 0), zs, 2, right)
                push(whole(zs, duo, -1), zs, 3, inner)
                arrived(whole(zs, duo, 1), ag_recv.at[zs, 1])
                push(part(zs, duo, 1, 1), zs, 2, left)
                push(whole(zs, duo, 1), zs, 3, inner)

            feed(it)

            @pl.when((it >= 2) & (it < NZ + 2))
            def _():
                zs = column(it - 2)
                arrived(whole(zs, duo, 2), ag_recv.at[zs, 2])
                push(whole(zs, duo, 2), zs, 3, inner)

            @pl.when((it >= 3) & (it < NZ + 3))
            def _():
                zs = column(it - 3)
                arrived(g_all.at[zs, 1 - duo], ag_recv.at[zs, 3])

            x_stages(it)

    @pl.when(core == 1)
    def _():
        @pl.loop(0, NZ + 6)
        def _(it):
            @pl.when(it < NZ)
            def _():
                zs = column(it)
                landed(it)
                push(whole(zs, duo, 0), zs, 3, inner)
                push(whole(zs, duo, 0), zs, 0, right)
                push(whole(zs, duo, 0), zs, 1, left)

            @pl.when((it >= 1) & (it < NZ + 1))
            def _():
                zs = column(it - 1)
                arrived(whole(zs, 1 - duo, 0), ag_recv.at[zs, 3])
                push(whole(zs, 1 - duo, 0), zs, 4, right)
                push(whole(zs, 1 - duo, 0), zs, 5, left)
                arrived(whole(zs, duo, -1), ag_recv.at[zs, 0])
                push(part(zs, duo, -1, 0), zs, 2, right)
                arrived(whole(zs, duo, 1), ag_recv.at[zs, 1])
                push(part(zs, duo, 1, 1), zs, 2, left)

            feed(it)

            @pl.when((it >= 2) & (it < NZ + 2))
            def _():
                zs = column(it - 2)
                arrived(whole(zs, 1 - duo, -1), ag_recv.at[zs, 4])
                push(part(zs, 1 - duo, -1, 0), zs, 6, right)
                arrived(whole(zs, 1 - duo, 1), ag_recv.at[zs, 5])
                push(part(zs, 1 - duo, 1, 1), zs, 6, left)
                arrived(whole(zs, duo, 2), ag_recv.at[zs, 2])

            @pl.when((it >= 3) & (it < NZ + 3))
            def _():
                zs = column(it - 3)
                arrived(whole(zs, 1 - duo, 2), ag_recv.at[zs, 6])

            x_stages(it)
    multiply(2 * NZ - 1, final=True)
    norms[d, 1:2] = jnp.sum(grad_sq[...], axis=0, keepdims=True)
    grad[:, pl.ds(pl.multiple_of(me * quarter, quarter), quarter)] = acc[pl.ds(me * rows, rows), :]

    @pl.loop(1, ND)
    def _(p):
        send(norms.at[d], norms.at[d], norm_send, norm_recv, z, (d + p) % ND)
    mates = (
        (me, d),
        (side * 2 + 1 - core, pal),
        ((1 - side) * 2 + core, outer),
        ((1 - side) * 2 + 1 - core, outer + 1 - 2 * core),
    )

    def columns(k):
        return pl.ds(pl.multiple_of(mates[k][0] * quarter, quarter), quarter)

    for k in range(1, 4):
        send(
            acc.at[pl.ds(mates[k][0] * rows, rows)],
            grad.at[:, columns(0)],
            half_send,
            half_recv.at[k - 1],
            z,
            mates[k][1],
        )

    def block_out(j):
        send(tag.at[j], got_tag.at[d], tag_send, tag_recv, z, j)
        send(
            bg_hbm.at[0, 0, pl.ds(2 * j, 2)],
            got.at[pl.ds(2 * d, 2)],
            bg_send,
            bg_recv,
            z,
            j,
        )

    near = ND // 2
    m_load.wait()

    arrived(norms.at[0 : ND - 1], norm_recv)
    totals = jnp.sum(norms[...], axis=0)
    weight_total = jnp.sum(totals[0:1], keepdims=True)
    grad_total = jnp.sum(totals[1:2], keepdims=True)
    weight_norm = jnp.sqrt(weight_total + eps_norm)
    trust = weight_norm / (jnp.sqrt(grad_total + eps_norm) + tower_decay * weight_norm)
    scale = tower_rate * trust

    strip = 16
    up = (z + 1) % NZ
    down = (z + NZ - 1) % NZ

    cut = rows // 2

    def piece(s, k, r):
        return slabs.at[s, mates[k][0], pl.ds(r * cut, cut)]

    def pass_on(s, k, r, way, hop):
        send(
            piece(s, k, r),
            piece(s, k, r),
            wz_send,
            wz_recv.at[way, hop, 2 * k + r],
            (up, down)[way],
            d,
        )

    def came(s, k, r, way, hop):
        arrived(piece(s, k, r), wz_recv.at[way, hop, 2 * k + r])

    def renew(k):
        for r in range(2):

            @pl.loop(0, cut // strip)
            def _(i):
                at = pl.ds(pl.multiple_of(r * cut + i * strip, strip), strip)
                old = w[0, at, columns(k)]
                new_m = momentum_keep * m[0, at, columns(k)] + scale * (
                    grad[at, columns(k)] + tower_decay * old
                )
                new_w = old - new_m
                m[0, at, columns(k)] = new_m
                w[0, at, columns(k)] = new_w
                slabs[z, mates[k][0], at, :] = new_w.astype(jnp.bfloat16)

            for way in range(2):
                pass_on(z, k, r, way, 0)

    def onward(j, ks):
        for k in ks:
            for r in range(2):
                for way in range(2):
                    if j < 3 or k % 2 == way:
                        s = ((z + NZ - j) % NZ, (z + j) % NZ)[way]
                        came(s, k, r, way, j - 1)
                        pass_on(s, k, r, way, j)
    renew(0)
    arrived(grad.at[:, columns(1)], half_recv.at[0])
    renew(1)

    @pl.loop(1, near)
    def _(p):
        block_out(side * near + (d + p) % near)
    onward(1, (0,))
    arrived(grad.at[:, columns(2)], half_recv.at[1])
    renew(2)
    onward(1, (1,))
    onward(2, (0,))
    arrived(grad.at[:, columns(3)], half_recv.at[2])
    renew(3)
    @pl.loop(0, near)
    def _(p):
        block_out((1 - side) * near + (d + p) % near)
    onward(2, (1,))
    onward(1, (2, 3))
    onward(3, (0, 1))
    onward(2, (2, 3))
    onward(3, (2, 3))
    own_load.wait()
    t_load.wait()

    arrived(got.at[0 : 2 * (ND - 1)], bg_recv)
    arrived(got_tag.at[0 : ND - 1], tag_recv)
    nb = table.shape[1]
    wide = table.shape[3]
    lane = lax.broadcasted_iota(jnp.int32, (strip, wide), 1)
    same = lane % strip == lax.broadcasted_iota(jnp.int32, (strip, wide), 0)
    names = lane // strip

    @pl.loop(0, ND)
    def _(s):
        for r in range(2):
            hit = (got_tag[s, r : r + 1, :] == names) & same
            pick[2 * s + r] = jnp.where(hit, 1.0, 0.0).astype(jnp.bfloat16)

    turned[...] = pick[...].reshape(2 * ND * strip, wide).T

    @pl.loop(0, table.shape[2] // strip)
    def _(i):
        at = pl.ds(pl.multiple_of(i * strip, strip), strip)
        values = got[:, at, :].reshape(2 * ND * strip, wide)
        total = jnp.dot(turned[...], values, preferred_element_type=jnp.float32)
        sums[:, at, :] = total.reshape(nb, strip, wide)

    tags = got_tag[:, 0:2, :]
    for b in range(nb):
        hits = jnp.sum(jnp.where(tags == b, 1.0, 0.0), axis=(0, 1)).reshape(1, wide)
        flat = table[0, b]
        total = sums[b]
        w_norm = jnp.sqrt(jnp.sum(flat * flat, keepdims=True) + eps_norm)
        g_norm = jnp.sqrt(jnp.sum(total * total, keepdims=True) + eps_norm)
        block_trust = w_norm / (g_norm + table_decay * w_norm)
        moved = flat - table_rate * block_trust * (total + table_decay * flat)
        table[0, b] = jnp.where(hits > 0, moved, flat)
    for k in range(4):
        way = k % 2
        for r in range(2):
            came(((z + 3) % NZ, (z + NZ - 3) % NZ)[way], k, r, 1 - way, 2)
            came(far, k, r, way, 3)
    arrived(g_slot.at[0:6], gz_send)
    for k in range(3):
        arrived(g_slot.at[0, 0], go_send.at[k])
    arrived(g_other.at[0:7], gx_send)
    arrived(g_relay, gr_send)
    arrived(g_relay, gf_send)
    arrived(x_slot.at[0:6], xz_send)
    arrived(x_relay, xr_send)
    arrived(x_relay, xf_send)
    arrived(x_all.at[:, 0], xo_send)
    arrived(x_all.at[:, 0:2], xp_send)
    arrived(g_all.at[0:7], ag_send)
    arrived(acc.at[0 : 3 * rows], half_send)
    arrived(norms.at[0 : ND - 1], norm_send)
    arrived(got.at[0 : 2 * (ND - 1)], bg_send)
    arrived(tag.at[0 : ND - 1], tag_send)
    arrived(slabs.at[0:7], wz_send)


def finish_kernel(
    owner_hbm, slots, new_w, new_m, new_t, out, w_out, m_out, t_out, owner, sem, own_sem
):
    owner_load = pltpu.make_async_copy(owner_hbm, owner, own_sem)
    owner_load.start()
    copies = [
        pltpu.make_async_copy(new_w, w_out, sem.at[4 * NZ]),
        pltpu.make_async_copy(new_m, m_out, sem.at[4 * NZ + 1]),
        pltpu.make_async_copy(new_t, t_out, sem.at[4 * NZ + 2]),
    ]
    for copy in copies:
        copy.start()
    owner_load.wait()
    wide = slots.shape[3]
    for l in range(NZ):
        for q in range(4):
            copy = pltpu.make_async_copy(
                slots.at[owner[l], q],
                out.at[l, :, q * wide : (q + 1) * wide],
                sem.at[4 * l + q],
            )
            copy.start()
            copies.append(copy)
    for copy in copies:
        copy.wait()


def local(
    layer_inputs,
    output_grads,
    layer_owner,
    master_weights,
    momentum,
    table_blocks,
    block_grads,
    block_ids,
    block_counts,
):
    layers, tokens, rows = layer_inputs.shape
    per, cols = output_grads.shape[1:]
    quarter = cols // 4
    nb, tall, wide = table_blocks.shape[1:]
    f32, bf16, i32 = jnp.float32, jnp.bfloat16, jnp.int32
    hbm = pl.BlockSpec(memory_space=pltpu.HBM)
    anywhere = pl.BlockSpec(memory_space=pl.ANY)
    dma = pltpu.SemaphoreType.DMA
    slots, new_w, new_m, new_t = pl.pallas_call(
        step_kernel,
        name="step",
        out_shape=(
            pltpu.VMEM((NZ, 4, rows, quarter), bf16),
            pltpu.VMEM(master_weights.shape, f32),
            pltpu.VMEM(momentum.shape, f32),
            pltpu.VMEM(table_blocks.shape, f32),
        ),
        in_specs=[hbm] * 9,
        out_specs=(pl.BlockSpec(memory_space=pltpu.VMEM),) * 4,
        scratch_shapes=[
            pltpu.VMEM((layers, tokens, rows), bf16),
            pltpu.VMEM((layers, NY, rows, tokens // NY), bf16),
            pltpu.VMEM((NZ, 4, NY, rows, tokens // NY), bf16),
            pltpu.VMEM((2, 2, rows, tokens // NY), bf16),
            pltpu.VMEM((layers, per, cols), bf16),
            pltpu.VMEM((layers, 4, per, quarter), bf16),
            pltpu.VMEM((layers, 2, per, quarter), bf16),
            pltpu.VMEM((NZ, 2, 2, NX, 2 * per, quarter), bf16),
            pltpu.VMEM((2, 2, per, quarter), bf16),
            pltpu.VMEM((4 * rows, quarter), f32),
            pltpu.VMEM((rows, cols), f32),
            pltpu.VMEM((nb, tall, wide), f32),
            pltpu.VMEM((2 * ND, wide // nb, wide), bf16),
            pltpu.VMEM((wide, 2 * ND * (wide // nb)), bf16),
            pltpu.VMEM((2 * ND, tall, wide), bf16),
            pltpu.VMEM((ND, 8, wide), i32),
            pltpu.VMEM((ND, 8, wide), i32),
            pltpu.VMEM((ND, 2, 128), f32),
            pltpu.VMEM((8, 128), f32),
            pltpu.SMEM(layer_owner.shape, i32),
            pltpu.SMEM(block_ids.shape, i32),
            pltpu.SMEM(block_counts.shape, i32),
            dma((9,)),
            dma,
            dma((NZ,)),
            dma((3,)),
            dma,
            dma((NZ,)),
            dma,
            dma((2,)),
            dma,
            dma,
            dma((NZ, 2)),
            dma,
            dma((2, 2)),
            dma,
            dma,
            dma((NZ, 2)),
            dma,
            dma((NZ, 2)),
            dma,
            dma((NZ, 7)),
            dma,
            dma((3,)),
            dma,
            dma,
            dma,
            dma,
            dma,
            dma,
            dma,
            dma((2, 4, 8)),
        ],
        compiler_params=pltpu.CompilerParams(
            collective_id=0, has_side_effects=True, vmem_limit_bytes=60_160_000
        ),
    )(
        layer_owner,
        block_ids,
        block_counts,
        layer_inputs,
        output_grads,
        master_weights,
        momentum,
        table_blocks,
        block_grads,
    )
    new_weights, new_master, new_moment, new_table = pl.pallas_call(
        finish_kernel,
        name="finish",
        in_specs=[anywhere] * 5,
        out_specs=(hbm,) * 4,
        scratch_shapes=[pltpu.SMEM(layer_owner.shape, i32), dma((4 * NZ + 3,)), dma],
        out_shape=(
            jax.ShapeDtypeStruct((layers, rows, cols), bf16),
            jax.ShapeDtypeStruct(master_weights.shape, f32),
            jax.ShapeDtypeStruct(momentum.shape, f32),
            jax.ShapeDtypeStruct(table_blocks.shape, f32),
        ),
        compiler_params=pltpu.CompilerParams(vmem_limit_bytes=1024 * 1024),
    )(layer_owner, slots, new_w, new_m, new_t)
    return new_master, new_moment, new_weights, new_table


def solution(mesh):
    return jax.shard_map(
        local,
        mesh=mesh,
        in_specs=(
            P(None, "grp", "dev"),
            P(None, ("grp", "dev"), None),
            P(),
            P("grp", "dev", None),
            P("grp", "dev", None),
            P("grp", "dev", None, None),
            P("grp", "dev", None, None, None),
            P("grp", "dev", None),
            P("grp", "dev", None),
        ),
        out_specs=(
            P("grp", "dev", None),
            P("grp", "dev", None),
            P(None, "dev", None),
            P("grp", "dev", None, None),
        ),
        check_vma=False,
    )
```

```python
import functools

import jax
import jax.numpy as jnp
from jax import lax
from jax.experimental import pallas as pl
from jax.experimental.pallas import tpu as pltpu
from jax.sharding import PartitionSpec as P

tower_rate = 0.5
momentum_keep = 0.9
tower_decay = 0.1
table_rate = 0.5
table_decay = 0.2
eps_norm = 1e-06

NZ = 8
NX = 4
NY = 4
ND = NX * NY * 2


def step_kernel(
    owner_hbm,
    ids_hbm,
    counts_hbm,
    x_hbm,
    g_hbm,
    w_hbm,
    m_hbm,
    t_hbm,
    bg_hbm,
    slabs,
    w,
    m,
    table,
    x_in,
    x_slot,
    x_all,
    x_relay,
    g_in,
    g_slot,
    g_other,
    g_all,
    g_relay,
    acc,
    grad,
    sums,
    pick,
    turned,
    got,
    tag,
    got_tag,
    norms,
    grad_sq,
    owner,
    ids,
    counts,
    in_sem,
    gz_send,
    gz_recv,
    go_send,
    gx_send,
    gx_recv,
    gr_send,
    gr_recv,
    gf_send,
    xz_send,
    xz_recv,
    xr_send,
    xr_recv,
    xf_send,
    xo_send,
    xo_recv,
    xp_send,
    xp_recv,
    ag_send,
    ag_recv,
    half_send,
    half_recv,
    norm_send,
    norm_recv,
    bg_send,
    bg_recv,
    tag_send,
    tag_recv,
    wz_send,
    wz_recv,
):
    z = lax.axis_index("grp")
    d = lax.axis_index("dev")
    core = d % 2
    cx = (d // 2) % NX
    cy = d // (2 * NX)
    chip = d // 2
    side = cy // 2
    duo = ((cy + 1) // 2) % 2
    oy = NY - 1 - cy
    iy = cy + 1 - 2 * (cy % 2)
    me = side * 2 + core
    pal = chip * 2 + 1 - core
    outer = (oy * NX + cx) * 2 + core
    inner = (iy * NX + cx) * 2 + core
    right = (cy * NX + (cx + 1) % NX) * 2 + core
    left = (cy * NX + (cx + NX - 1) % NX) * 2 + core
    rows = w_hbm.shape[1]
    cols = w_hbm.shape[2]
    quarter = cols // 4
    per = g_hbm.shape[1]
    tokens = x_hbm.shape[1]
    band = tokens // NY

    def send(src, dst, s_sem, r_sem, zz, dd):
        pltpu.make_async_remote_copy(
            src_ref=src,
            dst_ref=dst,
            send_sem=s_sem,
            recv_sem=r_sem,
            device_id=(zz, dd),
            device_id_type=pl.DeviceIdType.MESH,
        ).start()

    def arrived(ref, sem):
        pltpu.make_async_copy(ref, ref, sem).wait()

    def column(i):
        off = (i % 2) * ((i + 1) // 2) + (1 - i % 2) * (NZ - i // 2)
        return (z + off) % NZ

    g_load = pltpu.make_async_copy(g_hbm, g_in, in_sem.at[1])
    x_load = pltpu.make_async_copy(x_hbm, x_in, in_sem.at[0])
    w_load = pltpu.make_async_copy(w_hbm.at[0], w.at[0], in_sem.at[2])
    m_load = pltpu.make_async_copy(m_hbm.at[0], m.at[0], in_sem.at[3])
    t_load = pltpu.make_async_copy(t_hbm.at[0], table.at[0], in_sem.at[4])
    own_load = pltpu.make_async_copy(
        bg_hbm.at[0, 0, pl.ds(2 * d, 2)], got.at[pl.ds(2 * d, 2)], in_sem.at[5]
    )
    owner_load = pltpu.make_async_copy(owner_hbm, owner, in_sem.at[6])
    ids_load = pltpu.make_async_copy(ids_hbm, ids, in_sem.at[7])
    counts_load = pltpu.make_async_copy(counts_hbm, counts, in_sem.at[8])
    owner_load.start()
    g_load.start()
    barrier = pltpu.get_barrier_semaphore()

    @pl.loop(1, ND)
    def _(p):
        pl.semaphore_signal(
            barrier, inc=1, device_id=(z, (d + p) % ND), device_id_type=pl.DeviceIdType.MESH
        )

    @pl.loop(1, NZ)
    def _(p):
        for cc in range(2):
            pl.semaphore_signal(
                barrier,
                inc=1,
                device_id=((z + p) % NZ, chip * 2 + cc),
                device_id_type=pl.DeviceIdType.MESH,
            )

    x_load.start()
    w_load.start()
    m_load.start()
    t_load.start()
    own_load.start()
    ids_load.start()
    counts_load.start()

    def layer_of(s):
        found = jnp.int32(0)
        for l in range(NZ):
            found = jnp.where(owner[l] == s, l, found)
        return found
    owner_load.wait()
    g_load.wait()

    @pl.loop(0, NZ)
    def _(s):
        l = layer_of(s)
        for q in range(4):
            g_slot[s, q] = g_in[l, :, q * quarter : (q + 1) * quarter]

    g_all[z, duo, side, cx, pl.ds(core * per, per), :] = g_slot[z, me]
    pl.semaphore_wait(barrier, ND - 1 + 2 * (NZ - 1))
    def g_home(zs):
        return g_all.at[zs, duo, side, cx, pl.ds(core * per, per)]

    far = (z + NZ // 2) % NZ
    ways = (1, NZ - 1)
    there = (1 - side) * 2 + core
    mine = pl.ds(2 * side, 2)
    theirs = pl.ds(2 * (1 - side), 2)

    def g_there(zs):
        return g_all.at[zs, duo, 1 - side, cx, pl.ds(core * per, per)]

    send(g_slot.at[z, side * 2 + 1 - core], g_home(z), go_send.at[0], gz_recv.at[z], z, pal)
    for cc in range(2):
        send(
            g_slot.at[z, (1 - side) * 2 + cc],
            g_home(z),
            go_send.at[1 + cc],
            gz_recv.at[z],
            z,
            (oy * NX + cx) * 2 + cc,
        )

    def g_cross(zt):
        send(g_slot.at[zt, theirs], g_other.at[zt], gx_send, gx_recv.at[zt], z, outer)

    g_cross((z + 1) % NZ)
    g_cross((z + NZ - 1) % NZ)
    g_cross(far)
    for j in (2, 3):
        g_cross((z + j) % NZ)
        g_cross((z + NZ - j) % NZ)

    send(g_slot.at[far, mine], g_relay.at[0], gr_send, gr_recv.at[0], (z + 1) % NZ, d)
    def g_own(j):
        for zt in ((z + j) % NZ, (z + NZ - j) % NZ):
            for cc in range(2):
                send(
                    g_slot.at[zt, 2 * side + cc],
                    g_home(z),
                    gz_send,
                    gz_recv.at[z],
                    zt,
                    chip * 2 + cc,
                )

    def g_for_other(j):
        for zt in ((z + j) % NZ, (z + NZ - j) % NZ):
            arrived(g_other.at[zt], gx_recv.at[zt])
            for cc in range(2):
                send(
                    g_other.at[zt, cc], g_there(z), gz_send, gz_recv.at[z], zt, chip * 2 + cc
                )

    def x_out(j):
        for h in range(2):
            for zt in ((z + j) % NZ, (z + NZ - j) % NZ):
                at = pl.ds(2 * h, 2)
                send(
                    x_slot.at[zt, at], x_all.at[z, me, at], xz_send, xz_recv.at[z, h], zt, d
                )

    def x_half(zs, s, h):
        return x_all.at[zs, s, pl.ds(2 * h, 2)]

    def x_share(zs, h):
        ref = x_half(zs, me, h)
        send(ref, ref, xo_send, xo_recv.at[zs, h], z, outer)
        send(ref, ref, xp_send, xp_recv.at[zs, h], z, pal)

    def x_first(j, h):
        for zs in ((z + j) % NZ, (z + NZ - j) % NZ):
            arrived(x_half(zs, me, h), xz_recv.at[zs, h])
            x_share(zs, h)

    def x_first_far(h):
        arrived(x_half(far, me, h), xz_recv.at[far, h])
        x_share(far, h)

    def x_second(zs, h):
        ref = x_half(zs, there, h)
        arrived(ref, xo_recv.at[zs, h])
        send(ref, ref, xp_send, xp_recv.at[zs, h], z, pal)

    def x_second_both(j, h):
        for zs in ((z + j) % NZ, (z + NZ - j) % NZ):
            x_second(zs, h)

    g_own(1)
    g_own(2)

    x_load.wait()

    @pl.loop(0, NZ)
    def _(s):
        l = layer_of(s)
        for y in range(NY):
            x_slot[s, y] = x_in[l, y * band : (y + 1) * band, :].T

    x_all[z, me] = x_slot[z]

    for way in range(2):
        for h in range(2):
            send(
                x_slot.at[far, 2 * h + way],
                x_relay.at[way, h],
                xr_send,
                xr_recv.at[way, h],
                (z + ways[way]) % NZ,
                d,
            )

    for h in range(2):
        x_share(z, h)

    def whole(zs, pr, da):
        return g_all.at[zs, pr, :, (cx + da + NX) % NX]

    def part(zs, pr, da, h):
        return g_all.at[zs, pr, h, (cx + da + NX) % NX]

    pair_of = x_slot.at[0]

    def push(ref, zs, k, dd):
        send(ref, ref, ag_send, ag_recv.at[zs, k], z, dd)

    def landed(it):
        zs = column(it)

        @pl.when(it == 0)
        def _():
            arrived(g_slot.at[0, 0:3], gz_recv.at[zs])

        @pl.when(it > 0)
        def _():
            arrived(g_slot.at[0], gz_recv.at[zs])

    def feed(it):
        @pl.when(it == 0)
        def _():
            g_for_other(1)
            x_out(1)
            arrived(g_other.at[far], gx_recv.at[far])
            send(g_other.at[far], g_relay.at[1], gr_send, gr_recv.at[1], (z + NZ - 1) % NZ, d)

        @pl.when(it == 1)
        def _():
            g_for_other(2)
            g_own(3)
            g_for_other(3)
            x_out(2)

        @pl.when(it == 2)
        def _():
            relay()

    def relay():
        for way in range(2):
            zs = (z + NZ - ways[way]) % NZ
            zt = (zs + NZ // 2) % NZ
            arrived(g_relay.at[way], gr_recv.at[way])
            home = g_home(zs) if way == 0 else g_there(zs)
            sem = gz_recv.at[zs]
            for cc in range(2):
                send(g_relay.at[way, cc], home, gf_send, sem, zt, chip * 2 + cc)

        x_out(3)
        for way in range(2):
            zs = (z + NZ - ways[way]) % NZ
            zt = (zs + NZ // 2) % NZ
            for h in range(2):
                arrived(x_relay.at[way, h], xr_recv.at[way, h])
                send(
                    x_relay.at[way, h],
                    x_all.at[zs, me, 2 * h + way],
                    xf_send,
                    xz_recv.at[zs, h],
                    zt,
                    d,
                )

    def multiply(u, final=False):
        k = u // 2
        h = u % 2
        zs = column(k)
        arrived(x_slot.at[0], xp_recv.at[zs, h])
        @pl.loop(0, quarter // 256)
        def _(n):
            where = pl.ds(pl.multiple_of(n * 256, 256), 256)
            total = acc[:, where]
            for pr in range(2):
                y = pr + h * (NY - 1 - 2 * pr)
                total = total + jnp.dot(
                    x_all[zs, :, y].reshape(4 * rows, band),
                    g_all[zs, pr, h, :, :, where].reshape(band, 256),
                    preferred_element_type=jnp.float32,
                )
            acc[:, where] = total
            if final:
                squares = jnp.sum((total * total).reshape(4 * rows // 8, 8, 256), axis=0)
                grad_sq[...] += squares[:, :128] + squares[:, 128:]

    def x_stages(it):
        @pl.when(it == 2)
        def _():
            for h in range(2):
                x_second(z, h)

        def event(steps, do):
            for when, *what in steps:

                @pl.when(it == when)
                def _():
                    do(*what)

        event(
            ((3, 1, 0), (4, 1, 1), (5, 2, 0), (6, 2, 1), (8, 3, 0), (9, 3, 1)),
            x_first,
        )
        event(
            ((5, 1, 0), (6, 1, 1), (7, 2, 0), (8, 2, 1), (10, 3, 0), (11, 3, 1)),
            x_second_both,
        )
        event(((10, 0), (10, 1)), x_first_far)
        event(((12, far, 0), (13, far, 1)), x_second)

        first = jnp.where(
            it < 7, 0, jnp.where(it < 12, 2 * it - 12, it + 1)
        )
        count = jnp.where(
            it == 11, 3, jnp.where(it >= 12, 1, jnp.where((it == 4) | (it >= 7), 2, 0))
        )

        @pl.loop(first, first + count)
        def _(v):
            multiply(v + jnp.where(v == 11, 1, 0) - jnp.where(v == 12, 1, 0))
    ids_load.wait()
    counts_load.wait()

    @pl.loop(0, ND)
    def _(j):
        for r in range(2):
            t = jnp.where(r < counts[0, 0, j], ids[0, 0, 2 * j + r], -1)
            tag[j, r : r + 1, :] = jnp.full((1, tag.shape[2]), t, jnp.int32)

    got_tag[d] = tag[d]
    acc[...] = jnp.zeros_like(acc)
    w_load.wait()

    def weight_step(i, total):
        v = w[0, pl.ds(pl.multiple_of(i * 8, 8), 8), :]
        v = v * v
        for k in range(cols // 128):
            total = total + v[:, k * 128 : (k + 1) * 128]
        return total

    weight_sq = lax.fori_loop(0, rows // 8, weight_step, jnp.zeros((8, 128), jnp.float32))
    norms[d, 0:1] = jnp.sum(weight_sq, axis=0, keepdims=True)
    grad_sq[...] = jnp.zeros_like(grad_sq)
    @pl.when(core == 0)
    def _():
        @pl.loop(0, NZ + 6)
        def _(it):
            @pl.when(it < NZ)
            def _():
                zs = column(it)
                landed(it)
                push(whole(zs, duo, 0), zs, 0, right)
                push(whole(zs, duo, 0), zs, 0, left)
                push(whole(zs, duo, 0), zs, 3, inner)

            @pl.when((it >= 1) & (it < NZ + 1))
            def _():
                zs = column(it - 1)
                arrived(pair_of, ag_recv.at[zs, 0])
                push(part(zs, duo, -1, 0), zs, 2, right)
                push(part(zs, duo, 1, 1), zs, 2, left)
                push(whole(zs, duo, -1), zs, 3, inner)
                push(whole(zs, duo, 1), zs, 3, inner)

            feed(it)

            @pl.when((it >= 2) & (it < NZ + 2))
            def _():
                zs = column(it - 2)
                arrived(whole(zs, duo, 2), ag_recv.at[zs, 2])
                push(whole(zs, duo, 2), zs, 3, inner)

            @pl.when((it >= 3) & (it < NZ + 3))
            def _():
                zs = column(it - 3)
                arrived(g_all.at[zs, 1 - duo], ag_recv.at[zs, 3])

            x_stages(it)

    @pl.when(core == 1)
    def _():
        @pl.loop(0, NZ + 6)
        def _(it):
            @pl.when(it < NZ)
            def _():
                zs = column(it)
                landed(it)
                push(whole(zs, duo, 0), zs, 3, inner)
                push(whole(zs, duo, 0), zs, 0, right)
                push(whole(zs, duo, 0), zs, 0, left)

            @pl.when((it >= 1) & (it < NZ + 1))
            def _():
                zs = column(it - 1)
                arrived(whole(zs, 1 - duo, 0), ag_recv.at[zs, 3])
                push(whole(zs, 1 - duo, 0), zs, 1, right)
                push(whole(zs, 1 - duo, 0), zs, 1, left)
                arrived(pair_of, ag_recv.at[zs, 0])
                push(part(zs, duo, -1, 0), zs, 2, right)
                push(part(zs, duo, 1, 1), zs, 2, left)

            feed(it)

            @pl.when((it >= 2) & (it < NZ + 2))
            def _():
                zs = column(it - 2)
                arrived(pair_of, ag_recv.at[zs, 1])
                push(part(zs, 1 - duo, -1, 0), zs, 4, right)
                push(part(zs, 1 - duo, 1, 1), zs, 4, left)
                arrived(whole(zs, duo, 2), ag_recv.at[zs, 2])

            @pl.when((it >= 3) & (it < NZ + 3))
            def _():
                zs = column(it - 3)
                arrived(whole(zs, 1 - duo, 2), ag_recv.at[zs, 4])

            x_stages(it)
    multiply(2 * NZ - 1, final=True)
    norms[d, 1:2] = jnp.sum(grad_sq[...], axis=0, keepdims=True)
    grad[:, pl.ds(pl.multiple_of(me * quarter, quarter), quarter)] = acc[pl.ds(me * rows, rows), :]

    @pl.loop(1, ND)
    def _(p):
        send(norms.at[d], norms.at[d], norm_send, norm_recv, z, (d + p) % ND)
    mates = (
        (me, d),
        (side * 2 + 1 - core, pal),
        ((1 - side) * 2 + core, outer),
        ((1 - side) * 2 + 1 - core, outer + 1 - 2 * core),
    )

    def columns(k):
        return pl.ds(pl.multiple_of(mates[k][0] * quarter, quarter), quarter)

    for k in range(1, 4):
        send(
            acc.at[pl.ds(mates[k][0] * rows, rows)],
            grad.at[:, columns(0)],
            half_send,
            half_recv.at[k - 1],
            z,
            mates[k][1],
        )

    def block_out(j):
        send(tag.at[j], got_tag.at[d], tag_send, tag_recv, z, j)
        send(
            bg_hbm.at[0, 0, pl.ds(2 * j, 2)],
            got.at[pl.ds(2 * d, 2)],
            bg_send,
            bg_recv,
            z,
            j,
        )

    near = ND // 2
    m_load.wait()

    arrived(norms.at[0 : ND - 1], norm_recv)
    totals = jnp.sum(norms[...], axis=0)
    weight_total = jnp.sum(totals[0:1], keepdims=True)
    grad_total = jnp.sum(totals[1:2], keepdims=True)
    weight_norm = jnp.sqrt(weight_total + eps_norm)
    trust = weight_norm / (jnp.sqrt(grad_total + eps_norm) + tower_decay * weight_norm)
    scale = tower_rate * trust

    strip = 16
    up = (z + 1) % NZ
    down = (z + NZ - 1) % NZ

    cut = rows // 2

    def piece(s, k, r):
        return slabs.at[s, mates[k][0], pl.ds(r * cut, cut)]

    def pass_on(s, k, r, way, hop):
        send(
            piece(s, k, r),
            piece(s, k, r),
            wz_send,
            wz_recv.at[way, hop, k],
            (up, down)[way],
            d,
        )

    def came(s, k, way, hop):
        arrived(slabs.at[s, mates[k][0]], wz_recv.at[way, hop, k])

    def renew(k):
        for r in range(2):

            @pl.loop(0, cut // strip)
            def _(i):
                at = pl.ds(pl.multiple_of(r * cut + i * strip, strip), strip)
                old = w[0, at, columns(k)]
                new_m = momentum_keep * m[0, at, columns(k)] + scale * (
                    grad[at, columns(k)] + tower_decay * old
                )
                new_w = old - new_m
                m[0, at, columns(k)] = new_m
                w[0, at, columns(k)] = new_w
                slabs[z, mates[k][0], at, :] = new_w.astype(jnp.bfloat16)

            for way in range(2):
                pass_on(z, k, r, way, 0)

    def onward(j, ks):
        for k in ks:
            for way in range(2):
                if j < 3 or k % 2 == way:
                    s = ((z + NZ - j) % NZ, (z + j) % NZ)[way]
                    came(s, k, way, j - 1)
                    for r in range(2):
                        pass_on(s, k, r, way, j)
    renew(0)
    arrived(grad.at[:, columns(1)], half_recv.at[0])
    renew(1)

    @pl.loop(1, near)
    def _(p):
        block_out(side * near + (d + p) % near)
    onward(1, (0,))
    arrived(grad.at[:, columns(2)], half_recv.at[1])
    renew(2)
    onward(1, (1,))
    onward(2, (0,))
    arrived(grad.at[:, columns(3)], half_recv.at[2])
    renew(3)
    @pl.loop(0, near)
    def _(p):
        block_out((1 - side) * near + (d + p) % near)
    onward(2, (1,))
    onward(1, (2, 3))
    onward(3, (0, 1))
    onward(2, (2, 3))
    onward(3, (2, 3))
    own_load.wait()
    t_load.wait()

    arrived(got.at[0 : 2 * (ND - 1)], bg_recv)
    arrived(got_tag.at[0 : ND - 1], tag_recv)
    nb = table.shape[1]
    wide = table.shape[3]
    lane = lax.broadcasted_iota(jnp.int32, (strip, wide), 1)
    same = lane % strip == lax.broadcasted_iota(jnp.int32, (strip, wide), 0)
    names = lane // strip

    @pl.loop(0, ND)
    def _(s):
        for r in range(2):
            hit = (got_tag[s, r : r + 1, :] == names) & same
            pick[2 * s + r] = jnp.where(hit, 1.0, 0.0).astype(jnp.bfloat16)

    turned[...] = pick[...].reshape(2 * ND * strip, wide).T

    @pl.loop(0, table.shape[2] // strip)
    def _(i):
        at = pl.ds(pl.multiple_of(i * strip, strip), strip)
        values = got[:, at, :].reshape(2 * ND * strip, wide)
        total = jnp.dot(turned[...], values, preferred_element_type=jnp.float32)
        sums[:, at, :] = total.reshape(nb, strip, wide)

    tags = got_tag[:, 0:2, :]
    for b in range(nb):
        hits = jnp.sum(jnp.where(tags == b, 1.0, 0.0), axis=(0, 1)).reshape(1, wide)
        flat = table[0, b]
        total = sums[b]
        w_norm = jnp.sqrt(jnp.sum(flat * flat, keepdims=True) + eps_norm)
        g_norm = jnp.sqrt(jnp.sum(total * total, keepdims=True) + eps_norm)
        block_trust = w_norm / (g_norm + table_decay * w_norm)
        moved = flat - table_rate * block_trust * (total + table_decay * flat)
        table[0, b] = jnp.where(hits > 0, moved, flat)
    for k in range(4):
        way = k % 2
        came(((z + 3) % NZ, (z + NZ - 3) % NZ)[way], k, 1 - way, 2)
        came(far, k, way, 3)
    arrived(g_slot.at[0:6], gz_send)
    for k in range(3):
        arrived(g_slot.at[0, 0], go_send.at[k])
    arrived(g_other.at[0:7], gx_send)
    arrived(g_relay, gr_send)
    arrived(g_relay, gf_send)
    arrived(x_slot.at[0:6], xz_send)
    arrived(x_relay, xr_send)
    arrived(x_relay, xf_send)
    arrived(x_all.at[:, 0], xo_send)
    arrived(x_all.at[:, 0:2], xp_send)
    arrived(g_all.at[0:7], ag_send)
    arrived(acc.at[0 : 3 * rows], half_send)
    arrived(norms.at[0 : ND - 1], norm_send)
    arrived(got.at[0 : 2 * (ND - 1)], bg_send)
    arrived(tag.at[0 : ND - 1], tag_send)
    arrived(slabs.at[0:7], wz_send)


def finish_kernel(
    owner_hbm, slots, new_w, new_m, new_t, out, w_out, m_out, t_out, owner, sem, own_sem
):
    owner_load = pltpu.make_async_copy(owner_hbm, owner, own_sem)
    owner_load.start()
    copies = [
        pltpu.make_async_copy(new_w, w_out, sem.at[4 * NZ]),
        pltpu.make_async_copy(new_m, m_out, sem.at[4 * NZ + 1]),
        pltpu.make_async_copy(new_t, t_out, sem.at[4 * NZ + 2]),
    ]
    for copy in copies:
        copy.start()
    owner_load.wait()
    wide = slots.shape[3]
    for l in range(NZ):
        for q in range(4):
            copy = pltpu.make_async_copy(
                slots.at[owner[l], q],
                out.at[l, :, q * wide : (q + 1) * wide],
                sem.at[4 * l + q],
            )
            copy.start()
            copies.append(copy)
    for copy in copies:
        copy.wait()


def local(
    layer_inputs,
    output_grads,
    layer_owner,
    master_weights,
    momentum,
    table_blocks,
    block_grads,
    block_ids,
    block_counts,
):
    layers, tokens, rows = layer_inputs.shape
    per, cols = output_grads.shape[1:]
    quarter = cols // 4
    nb, tall, wide = table_blocks.shape[1:]
    f32, bf16, i32 = jnp.float32, jnp.bfloat16, jnp.int32
    hbm = pl.BlockSpec(memory_space=pltpu.HBM)
    anywhere = pl.BlockSpec(memory_space=pl.ANY)
    dma = pltpu.SemaphoreType.DMA
    slots, new_w, new_m, new_t = pl.pallas_call(
        step_kernel,
        name="step",
        out_shape=(
            pltpu.VMEM((NZ, 4, rows, quarter), bf16),
            pltpu.VMEM(master_weights.shape, f32),
            pltpu.VMEM(momentum.shape, f32),
            pltpu.VMEM(table_blocks.shape, f32),
        ),
        in_specs=[hbm] * 9,
        out_specs=(pl.BlockSpec(memory_space=pltpu.VMEM),) * 4,
        scratch_shapes=[
            pltpu.VMEM((layers, tokens, rows), bf16),
            pltpu.VMEM((layers, NY, rows, tokens // NY), bf16),
            pltpu.VMEM((NZ, 4, NY, rows, tokens // NY), bf16),
            pltpu.VMEM((2, 2, rows, tokens // NY), bf16),
            pltpu.VMEM((layers, per, cols), bf16),
            pltpu.VMEM((layers, 4, per, quarter), bf16),
            pltpu.VMEM((layers, 2, per, quarter), bf16),
            pltpu.VMEM((NZ, 2, 2, NX, 2 * per, quarter), bf16),
            pltpu.VMEM((2, 2, per, quarter), bf16),
            pltpu.VMEM((4 * rows, quarter), f32),
            pltpu.VMEM((rows, cols), f32),
            pltpu.VMEM((nb, tall, wide), f32),
            pltpu.VMEM((2 * ND, wide // nb, wide), bf16),
            pltpu.VMEM((wide, 2 * ND * (wide // nb)), bf16),
            pltpu.VMEM((2 * ND, tall, wide), bf16),
            pltpu.VMEM((ND, 8, wide), i32),
            pltpu.VMEM((ND, 8, wide), i32),
            pltpu.VMEM((ND, 2, 128), f32),
            pltpu.VMEM((8, 128), f32),
            pltpu.SMEM(layer_owner.shape, i32),
            pltpu.SMEM(block_ids.shape, i32),
            pltpu.SMEM(block_counts.shape, i32),
            dma((9,)),
            dma,
            dma((NZ,)),
            dma((3,)),
            dma,
            dma((NZ,)),
            dma,
            dma((2,)),
            dma,
            dma,
            dma((NZ, 2)),
            dma,
            dma((2, 2)),
            dma,
            dma,
            dma((NZ, 2)),
            dma,
            dma((NZ, 2)),
            dma,
            dma((NZ, 5)),
            dma,
            dma((3,)),
            dma,
            dma,
            dma,
            dma,
            dma,
            dma,
            dma,
            dma((2, 4, 4)),
        ],
        compiler_params=pltpu.CompilerParams(
            collective_id=0, has_side_effects=True, vmem_limit_bytes=60_160_000
        ),
    )(
        layer_owner,
        block_ids,
        block_counts,
        layer_inputs,
        output_grads,
        master_weights,
        momentum,
        table_blocks,
        block_grads,
    )
    new_weights, new_master, new_moment, new_table = pl.pallas_call(
        finish_kernel,
        name="finish",
        in_specs=[anywhere] * 5,
        out_specs=(hbm,) * 4,
        scratch_shapes=[pltpu.SMEM(layer_owner.shape, i32), dma((4 * NZ + 3,)), dma],
        out_shape=(
            jax.ShapeDtypeStruct((layers, rows, cols), bf16),
            jax.ShapeDtypeStruct(master_weights.shape, f32),
            jax.ShapeDtypeStruct(momentum.shape, f32),
            jax.ShapeDtypeStruct(table_blocks.shape, f32),
        ),
        compiler_params=pltpu.CompilerParams(vmem_limit_bytes=1024 * 1024),
    )(layer_owner, slots, new_w, new_m, new_t)
    return new_master, new_moment, new_weights, new_table


def solution(mesh):
    return jax.shard_map(
        local,
        mesh=mesh,
        in_specs=(
            P(None, "grp", "dev"),
            P(None, ("grp", "dev"), None),
            P(),
            P("grp", "dev", None),
            P("grp", "dev", None),
            P("grp", "dev", None, None),
            P("grp", "dev", None, None, None),
            P("grp", "dev", None),
            P("grp", "dev", None),
        ),
        out_specs=(
            P("grp", "dev", None),
            P("grp", "dev", None),
            P(None, "dev", None),
            P("grp", "dev", None, None),
        ),
        check_vma=False,
    )
```
